32 devices in a mesh: narrow: 4 (over x, core), wide: 8 (over z, y).
Axes of the slice: x: 2, y: 2, z: 4, core: 2. Of those that a mesh axis runs over, the one named last changes fastest.
Arguments:
- patches: bfloat16 [64, 512, 768], P(('narrow', 'wide')), may hold values from -6 to 6
- cotangent: bfloat16 [64, 512, 768], P(('narrow', 'wide')), may hold values from -6 to 6
- mask_index: int32 [64, 450], P(('narrow', 'wide')), may hold values from 0 to 511, as said below
- mask_count: int32 [64], P(('narrow', 'wide')), may hold values from 100 to 450
- mask_embed: bfloat16 [768], P('wide'), may hold values from -6 to 6
- ln1_gain: bfloat16 [768], P('wide'), may hold values from 0.5 to 1.5
- ln1_bias: bfloat16 [768], P('wide'), may hold values from -1.75 to 1.75
- w_qkv: bfloat16 [768, 2304], P('wide'), may hold values from -0.3125 to 0.3125
- bias_q: bfloat16 [768], P('wide'), may hold values from -1.75 to 1.75
- bias_v: bfloat16 [768], P('wide'), may hold values from -1.75 to 1.75
- w_out: bfloat16 [768, 768], P('wide'), may hold values from -0.625 to 0.625
- bias_out: bfloat16 [768], P('wide'), may hold values from -1.75 to 1.75
- ln2_gain: bfloat16 [768], P('wide'), may hold values from 0.5 to 1.5
- ln2_bias: bfloat16 [768], P('wide'), may hold values from -1.75 to 1.75
- w_fc1: bfloat16 [768, 3072], P('wide'), may hold values from -0.21875 to 0.21875
- bias_fc1: bfloat16 [3072], P('wide'), may hold values from -1.75 to 1.75
- w_fc2: bfloat16 [3072, 768], P('wide'), may hold values from -0.15625 to 0.15625
- bias_fc2: bfloat16 [768], P('wide'), may hold values from -1.75 to 1.75
Outputs:
- output: bfloat16 [64, 512, 768], P(('narrow', 'wide'))
- patch_grad: bfloat16 [64, 512, 768], P(('narrow', 'wide'))
- grad_mask_embed: float32 [768], P('wide')
- grad_ln1_gain: float32 [768], P('wide')
- grad_ln1_bias: float32 [768], P('wide')
- grad_w_qkv: float32 [768, 2304], P('wide')
- grad_bias_q: float32 [768], P('wide')
- grad_bias_v: float32 [768], P('wide')
- grad_w_out: float32 [768, 768], P('wide')
- grad_bias_out: float32 [768], P('wide')
- grad_ln2_gain: float32 [768], P('wide')
- grad_ln2_bias: float32 [768], P('wide')
- grad_w_fc1: float32 [768, 3072], P('wide')
- grad_bias_fc1: float32 [3072], P('wide')
- grad_w_fc2: float32 [3072, 768], P('wide')
- grad_bias_fc2: float32 [768], P('wide')
The draws below stay inside these ranges and needn't reach their ends.
Inputs may be any that keep to these rules, and one draw needn't show every extreme that they name: `mask_index`: row c holds 450 distinct patch numbers of clip c; its first mask_count[c] entries are the masked patches.
All inputs are finite; a program needn't handle non-finite values.
Results may differ from the reference program's by a relative error of at most 0.019.
Values may be sent and summed in bfloat16 or wider, within the bound.
A program may use at most 192 MiB of HBM per device.

```python
import jax
import jax.numpy as jnp
from jax import lax

D = 768
HEADS = 12
HD = 64
FF = 3072
SEQ = 512
MAXM = 450
MINM = 100
CLIPS = 64


def draw_mask_index(key, part):
    clip_keys = jax.random.split(jax.random.fold_in(key, 11), CLIPS)

    def one_clip(clip_key):
        return jax.random.permutation(clip_key, SEQ)[:MAXM]
    return jax.vmap(one_clip)(clip_keys).astype(jnp.int32)


def draw_mask_count(key, part):
    counts = jax.random.randint(jax.random.fold_in(key, 23), (CLIPS,), MINM, MAXM + 1)
    counts = counts.at[0].set(MAXM).at[CLIPS - 1].set(MINM)
    return counts.astype(jnp.int32)


def level_of(stream_key, dims, shards, smallest, high):
    def one(dim, parts):
        draws = jax.random.uniform(jax.random.fold_in(jax.random.fold_in(stream_key, 6), dim), (parts,), jnp.float32, smallest / len(shards), high / len(shards))
        return jnp.repeat(jnp.exp(draws), dims[dim] // parts).reshape((-1,) + (1,) * (len(dims) - dim - 1))

    factor_of = one(*shards[0])
    for cut in shards[1:]:
        factor_of = factor_of * one(*cut)
    return factor_of


def centred(own_key, extent, spread, reach, pieces=(), held_as=jnp.bfloat16):
    array = spread * jax.random.normal(own_key, extent, jnp.float32)
    if pieces:
        array = array * level_of(own_key, extent, pieces, -0.22, 0.18)
    return jnp.clip(array, -reach, reach).astype(held_as)


def setup_inputs(seed: int = 0) -> dict:
    arg_keys = jax.random.split(jax.random.key(seed), 19)
    patches = centred(arg_keys[0], (CLIPS, SEQ, D), 1.0, 6.0, ((0, 32),))
    cotangent = centred(arg_keys[1], (CLIPS, SEQ, D), 1.0, 6.0, ((0, 32),))
    mask_index = draw_mask_index(jax.random.fold_in(arg_keys[18], 71), 0)
    mask_count = draw_mask_count(jax.random.fold_in(arg_keys[18], 71), 0)
    mask_embed = centred(arg_keys[4], (D,), 1.0, 6.0, ((0, 8),))
    ln1_gain = jnp.clip(1.0 + 0.1 * jax.random.normal(arg_keys[5], (D,), jnp.float32), 0.5, 1.5).astype(jnp.bfloat16)
    ln1_bias = centred(arg_keys[6], (D,), 0.3, 1.75, ((0, 8),))
    w_qkv = centred(arg_keys[7], (D, 3 * D), (D // 2) ** -0.5, 0.3125, ((0, 8),))
    bias_q = centred(arg_keys[8], (D,), 0.3, 1.75, ((0, 8),))
    bias_v = centred(arg_keys[9], (D,), 0.3, 1.75, ((0, 8),))
    w_out = centred(arg_keys[10], (D, D), (D // 8) ** -0.5, 0.625, ((0, 8),))
    bias_out = centred(arg_keys[11], (D,), 0.3, 1.75, ((0, 8),))
    ln2_gain = jnp.clip(1.0 + 0.1 * jax.random.normal(arg_keys[12], (D,), jnp.float32), 0.5, 1.5).astype(jnp.bfloat16)
    ln2_bias = centred(arg_keys[13], (D,), 0.3, 1.75, ((0, 8),))
    w_fc1 = centred(arg_keys[14], (D, FF), D ** -0.5, 0.21875, ((0, 8),))
    bias_fc1 = centred(arg_keys[15], (FF,), 0.3, 1.75, ((0, 8),))
    w_fc2 = centred(arg_keys[16], (FF, D), (FF // 2) ** -0.5, 0.15625, ((0, 8),))
    bias_fc2 = centred(arg_keys[17], (D,), 0.3, 1.75, ((0, 8),))
    return {"patches": patches, "cotangent": cotangent, "mask_index": mask_index, "mask_count": mask_count, "mask_embed": mask_embed, "ln1_gain": ln1_gain, "ln1_bias": ln1_bias, "w_qkv": w_qkv, "bias_q": bias_q, "bias_v": bias_v, "w_out": w_out, "bias_out": bias_out, "ln2_gain": ln2_gain, "ln2_bias": ln2_bias, "w_fc1": w_fc1, "bias_fc1": bias_fc1, "w_fc2": w_fc2, "bias_fc2": bias_fc2}


@jax.custom_vjp
def low(v):
    return lax.optimization_barrier(v.astype(jnp.bfloat16)).astype(jnp.float32)

@jax.custom_vjp
def low_back(v):
    return v

def low_keep(v):
    return (low(v), None)

def low_pass(kept, grad):
    return (grad,)

def back_keep(v):
    return (v, None)

def back_low(kept, grad):
    return (low(grad),)
low.defvjp(low_keep, low_pass)
low_back.defvjp(back_keep, back_low)
epsilon = 1e-06
highest = lax.Precision.HIGHEST

def matmul_hi(left_side, right_side):
    return jnp.dot(left_side, right_side, precision=highest, preferred_element_type=jnp.float32)

def layer_norm(values, ln_gain, ln_shift):
    row_mean = lax.optimization_barrier(jnp.mean(values, axis=-1, keepdims=True))
    centered = values - row_mean
    variance = lax.optimization_barrier(jnp.mean(centered * centered, axis=-1, keepdims=True))
    return centered * lax.rsqrt(variance + epsilon) * ln_gain[None, :] + ln_shift[None, :]

def mask_table(mask_index, mask_count):
    slot_ids = jnp.arange(MAXM).astype(jnp.int32)
    valid_slots = slot_ids[None, :, None] < mask_count[:, None, None]
    patch_ids = jnp.arange(SEQ).astype(jnp.int32)
    hits = (mask_index[:, :, None] == patch_ids[None, None, :]) & valid_slots
    return lax.optimization_barrier(jnp.sum(hits.astype(jnp.float32), axis=1))

def layer_block(params, patch_rows, mask_rows):
    mask_embed, ln1_gain, ln1_bias, w_qkv, bias_q, bias_v, w_out, bias_out, ln2_gain, ln2_bias, w_fc1, bias_fc1, w_fc2, bias_fc2 = params
    group_size = patch_rows.shape[0]
    row_count = group_size * SEQ
    masked = mask_rows.reshape(row_count, 1)
    start_rows = patch_rows.reshape(row_count, D) * (1.0 - masked) + masked * mask_embed[None, :]
    attn_in = low(layer_norm(start_rows, ln1_gain, ln1_bias))
    qkv_bias = jnp.concatenate([bias_q, jnp.zeros_like(bias_q), bias_v])
    qkv = low(low_back(matmul_hi(attn_in, w_qkv) + qkv_bias[None, :]))
    split_qkv = qkv.reshape(group_size, SEQ, 3, HEADS, HD)
    query_rows = split_qkv[:, :, 0]
    key_rows = split_qkv[:, :, 1]
    value_rows = split_qkv[:, :, 2]
    scores = low_back(jnp.einsum('cqhd,ckhd->chqk', query_rows, key_rows, precision=highest) * HD ** (-0.5))
    soft_probs = low(jax.nn.softmax(scores, axis=-1))
    attn_mixed = jnp.einsum('chqk,ckhd->cqhd', soft_probs, value_rows, precision=highest).reshape(row_count, D)
    attn_mixed = low(low_back(attn_mixed))
    branch = low_back(matmul_hi(attn_mixed, w_out) + bias_out[None, :])
    middle = start_rows + branch
    mlp_in = low(layer_norm(middle, ln2_gain, ln2_bias))
    hidden = low_back(matmul_hi(mlp_in, w_fc1) + bias_fc1[None, :])
    activated = low(jax.nn.gelu(hidden, approximate=False))
    mlp_out = low_back(matmul_hi(activated, w_fc2) + bias_fc2[None, :])
    return (middle + mlp_out).reshape(group_size, SEQ, D)

def reference(patches, cotangent, mask_index, mask_count, mask_embed, ln1_gain, ln1_bias, w_qkv, bias_q, bias_v, w_out, bias_out, ln2_gain, ln2_bias, w_fc1, bias_fc1, w_fc2, bias_fc2):
    params = tuple((weight_item.astype(jnp.float32) for weight_item in (mask_embed, ln1_gain, ln1_bias, w_qkv, bias_q, bias_v, w_out, bias_out, ln2_gain, ln2_bias, w_fc1, bias_fc1, w_fc2, bias_fc2)))
    group_size = 8 if CLIPS % 8 == 0 else 1
    steps_count = CLIPS // group_size
    mask_all = mask_table(mask_index, mask_count).reshape(steps_count, group_size, SEQ)
    patch_all = patches.astype(jnp.float32).reshape(steps_count, group_size, SEQ, D)
    grad_all = cotangent.astype(jnp.float32).reshape(steps_count, group_size, SEQ, D)
    saved_block = jax.checkpoint(layer_block)

    def whole(params_in, patches_in):
        return lax.map(lambda block_pair: saved_block(params_in, block_pair[0], block_pair[1]), (patches_in, mask_all))
    result, pullback = jax.vjp(whole, params, patch_all)
    grad_params, grad_patches = pullback(grad_all)
    return (result.reshape(CLIPS, SEQ, D).astype(jnp.bfloat16), grad_patches.reshape(CLIPS, SEQ, D).astype(jnp.bfloat16), grad_params[0], grad_params[1], grad_params[2], grad_params[3], grad_params[4], grad_params[5], grad_params[6], grad_params[7], grad_params[8], grad_params[9], grad_params[10], grad_params[11], grad_params[12], grad_params[13])
```

```python
import functools
import jax
import jax.numpy as jnp
from jax import lax
from jax.experimental import pallas as pl
from jax.experimental.pallas import tpu as pltpu
from jax.sharding import PartitionSpec as P

HEADS = 12
HD = 64


epsilon = 1e-06
inv_root_two = 0.7071067811865476
inv_root_tau = 0.3989422804014327


def dot_rows(left_side, right_side):
    return lax.dot_general(
        left_side, right_side, (((0,), (0,)), ((), ())), preferred_element_type=jnp.float32
    )


def dot_back(left_side, right_side):
    return lax.dot_general(
        left_side, right_side, (((1,), (1,)), ((), ())), preferred_element_type=jnp.float32
    )


def norm_rows(values):
    row_mean = jnp.mean(values, axis=-1, keepdims=True)
    centered = values - row_mean
    variance = jnp.mean(centered * centered, axis=-1, keepdims=True)
    inv_std = lax.rsqrt(variance + epsilon)
    return (centered * inv_std, inv_std)


def norm_back(grad_in, normed, inv_std, ln_gain):
    grad_normed = grad_in * ln_gain[None, :]
    mean_grad = jnp.mean(grad_normed, axis=-1, keepdims=True)
    mean_cross = jnp.mean(grad_normed * normed, axis=-1, keepdims=True)
    return inv_std * (grad_normed - mean_grad - normed * mean_cross)


def split_heads(qkv_clip):
    seq_len = qkv_clip.shape[0]
    split_qkv = qkv_clip.reshape(seq_len, 3, HEADS, HD)
    return (split_qkv[:, 0], split_qkv[:, 1], split_qkv[:, 2])


def clip_scores(query_rows, key_rows):
    return jnp.einsum(
        "qhd,khd->hqk", query_rows, key_rows, preferred_element_type=jnp.float32
    ) * HD ** (-0.5)


def attend(qkv_clip):
    query_rows, key_rows, value_rows = split_heads(qkv_clip)
    scores = clip_scores(query_rows, key_rows)
    row_max = jnp.max(scores, axis=-1, keepdims=True)
    exp_scores = jnp.exp(scores - row_max)
    row_total = jnp.sum(exp_scores, axis=-1, keepdims=True)
    soft_probs = (exp_scores / row_total).astype(jnp.bfloat16)
    attn_mixed = jnp.einsum(
        "hqk,khd->qhd", soft_probs, value_rows, preferred_element_type=jnp.float32
    )
    log_total = (row_max + jnp.log(row_total))[..., 0]
    return (attn_mixed.reshape(qkv_clip.shape[0], HEADS * HD).astype(jnp.bfloat16), log_total)


def attend_back(block_args):
    qkv_clip, grad_mixed, log_total = block_args
    query_rows, key_rows, value_rows = split_heads(qkv_clip)
    grad_heads = grad_mixed.reshape(qkv_clip.shape[0], HEADS, HD)
    soft_probs = jnp.exp(clip_scores(query_rows, key_rows) - log_total[..., None])
    grad_probs = jnp.einsum(
        "qhd,khd->hqk", grad_heads, value_rows, preferred_element_type=jnp.float32
    )
    grad_value = jnp.einsum(
        "hqk,qhd->khd",
        soft_probs.astype(jnp.bfloat16),
        grad_heads,
        preferred_element_type=jnp.float32,
    )
    grad_scores = soft_probs * (
        grad_probs - jnp.sum(soft_probs * grad_probs, axis=-1, keepdims=True)
    )
    grad_scores = grad_scores.astype(jnp.bfloat16)
    grad_query = jnp.einsum(
        "hqk,khd->qhd", grad_scores, key_rows, preferred_element_type=jnp.float32
    ) * HD ** (-0.5)
    grad_key = jnp.einsum(
        "hqk,qhd->khd", grad_scores, query_rows, preferred_element_type=jnp.float32
    ) * HD ** (-0.5)
    stacked = jnp.stack([grad_query, grad_key, grad_value], axis=1)
    return stacked.reshape(qkv_clip.shape[0], 3 * HEADS * HD).astype(jnp.bfloat16)


MESH = pl.DeviceIdType.MESH
BF = jnp.bfloat16
F32 = jnp.float32

UNITS = (
    [("qkv", 768 * j, 0) for j in range(3)]
    + [("out", 0, 0)]
    + [("fc1", 768 * j, 0) for j in range(4)]
    + [("fc2", 0, 96 * j) for j in range(4)]
)
NU = len(UNITS)


def lanes(start):
    return pl.multiple_of(start, 128)


class Place:
    def __init__(self):
        n = lax.axis_index("narrow")
        w = lax.axis_index("wide")
        self.n, self.w = n, w
        self.core, self.x = n % 2, n // 2
        self.y, self.z = w % 2, w // 2
        self.core_peer = (self.x * 2 + (1 - self.core), w)
        self.x_peer = ((1 - self.x) * 2 + self.core, w)
        self.y_peer = (n, self.z * 2 + (1 - self.y))

    def z_up(self, k):
        return (self.z + k) % 4

    def z_peer(self, k):
        return (self.n, self.z_up(k) * 2 + self.y)

    def greet(self):
        barrier = pltpu.get_barrier_semaphore()
        peers = [self.core_peer, self.x_peer, self.y_peer] + [self.z_peer(k) for k in (1, 2, 3)]
        for peer in peers:
            pl.semaphore_signal(barrier, inc=1, device_id=peer, device_id_type=MESH)
        pl.semaphore_wait(barrier, len(peers))


def remote(src, dst, send, recv, peer):
    return pltpu.make_async_remote_copy(
        src_ref=src, dst_ref=dst, send_sem=send, recv_sem=recv, device_id=peer, device_id_type=MESH
    )


class Gather:
    SEMS = [
        pltpu.SemaphoreType.DMA((NU, 10)),
        pltpu.SemaphoreType.DMA((NU, 10)),
        pltpu.SemaphoreType.DMA((NU,)),
        pltpu.SemaphoreType.DMA((8,)),
        pltpu.SemaphoreType.DMA((8,)),
    ]

    def __init__(self, place, shards, full, small, small_full, send, recv, local, ssend, srecv):
        self.p, self.shards, self.full = place, shards, full
        self.small, self.small_full = small, small_full
        self.send, self.recv, self.local, self.ssend, self.srecv = send, recv, local, ssend, srecv
        self.sent = []

    def go(self, u, i, src, dst, peer):
        copy = remote(src, dst, self.send.at[u, i], self.recv.at[u, i], peer)
        copy.start()
        self.sent.append(copy)

    def arrived(self, u, i, dst):
        remote(dst, dst, self.send.at[u, i], self.recv.at[u, i], self.p.x_peer).wait_recv()

    def small_stage(self, stage):
        p = self.p
        if stage == 0:
            own = self.small_full.at[p.z, p.y]
            pltpu.make_async_copy(self.small, own, self.local.at[0]).start()
            pltpu.make_async_copy(self.small, own, self.local.at[0]).wait()
            for k in (1, 2, 3):
                copy = remote(self.small, own, self.ssend.at[k], self.srecv.at[k], p.z_peer(k))
                copy.start()
                self.sent.append(copy)
        elif stage == 1:
            for k in (1, 2, 3):
                dst = self.small_full.at[p.z_up(4 - k), p.y]
                remote(dst, dst, self.ssend.at[k], self.srecv.at[k], p.x_peer).wait_recv()
            mine = self.small_full.at[:, p.y]
            copy = remote(mine, mine, self.ssend.at[0], self.srecv.at[0], p.y_peer)
            copy.start()
            self.sent.append(copy)
        else:
            dst = self.small_full.at[:, 1 - p.y]
            remote(dst, dst, self.ssend.at[0], self.srecv.at[0], p.x_peer).wait_recv()

    def stage(self, u, stage):
        p = self.p
        name, co, ro = UNITS[u]
        full, shard = self.full[name], self.shards[name]
        rows = pl.ds(ro, 96)
        own = pl.ds(lanes(co + p.core * 384 + p.x * 128), 256)
        exc = pl.ds(lanes(co + p.core * 384 + p.x * 256), 128)
        peer_exc = pl.ds(lanes(co + p.core * 384 + (1 - p.x) * 256), 128)
        oth = pl.ds(lanes(co + (1 - p.core) * 384 + p.x * 128), 256)
        oth_exc = pl.ds(lanes(co + (1 - p.core) * 384 + (1 - p.x) * 256), 128)
        if stage == 0:
            mine = shard.at[rows, own]
            home = full.at[p.z, p.y, rows, own]
            pltpu.make_async_copy(mine, home, self.local.at[u]).start()
            for k in (1, 2, 3):
                self.go(u, k, mine, home, p.z_peer(k))
        elif stage == 1:
            home = full.at[p.z, p.y, rows, own]
            pltpu.make_async_copy(shard.at[rows, own], home, self.local.at[u]).wait()
            for k in (1, 2, 3):
                self.arrived(u, k, full.at[p.z_up(4 - k), p.y, rows, own])
            column = full.at[:, p.y, rows, own]
            part = full.at[:, p.y, rows, exc]
            self.go(u, 0, column, column, p.y_peer)
            self.go(u, 4, part, part, p.x_peer)
            self.go(u, 5, column, column, p.core_peer)
        elif stage == 2:
            column = full.at[:, 1 - p.y, rows, own]
            part = full.at[:, 1 - p.y, rows, exc]
            self.arrived(u, 0, column)
            self.go(u, 6, part, part, p.x_peer)
            self.go(u, 7, column, column, p.core_peer)
        elif stage == 3:
            self.arrived(u, 4, full.at[:, p.y, rows, peer_exc])
            self.arrived(u, 6, full.at[:, 1 - p.y, rows, peer_exc])
            both = full.at[:, :, rows, peer_exc]
            self.go(u, 8, both, both, p.core_peer)
        else:
            self.arrived(u, 5, full.at[:, p.y, rows, oth])
            self.arrived(u, 7, full.at[:, 1 - p.y, rows, oth])
            self.arrived(u, 8, full.at[:, :, rows, oth_exc])

    def finish(self):
        for copy in self.sent:
            copy.wait_send()


class Reduce:
    SCRATCH = [
        pltpu.VMEM((NU, 4, 2, 96, 384), BF),
        pltpu.VMEM((NU, 4, 2, 96, 128), BF),
        pltpu.VMEM((NU, 4, 96, 256), BF),
        pltpu.VMEM((NU, 3, 96, 256), BF),
        pltpu.VMEM((NU, 2, 96, 256), BF),
        pltpu.VMEM((NU, 2, 96, 384), BF),
        pltpu.VMEM((10, 16, 768), F32),
        pltpu.SemaphoreType.DMA((NU, 8)),
        pltpu.SemaphoreType.DMA((NU, 8)),
        pltpu.SemaphoreType.DMA((6,)),
        pltpu.SemaphoreType.DMA((6,)),
    ]

    def __init__(self, place, grads, outs, bufs):
        self.p, self.grads, self.outs = place, grads, outs
        (self.c, self.xb, self.yb, self.zb, self.f, self.e, self.s,
         self.send, self.recv, self.ssend, self.srecv) = bufs
        self.sent = []

    def go(self, u, i, src, dst, peer):
        copy = remote(src, dst, self.send.at[u, i], self.recv.at[u, i], peer)
        copy.start()
        self.sent.append(copy)

    def arrived(self, u, i, dst):
        remote(dst, dst, self.send.at[u, i], self.recv.at[u, i], self.p.x_peer).wait_recv()

    def stage(self, u, stage):
        p = self.p
        name, co, ro = UNITS[u]
        grad = self.grads[name]
        rows = pl.ds(ro, 96)
        own = pl.ds(lanes(co + p.core * 384), 384)
        oth = pl.ds(lanes(co + (1 - p.core) * 384), 384)
        exc = pl.ds(lanes(p.x * 256), 128)
        peer_exc = pl.ds(lanes((1 - p.x) * 256), 128)
        two = pl.ds(lanes(p.x * 128), 256)
        c, xb, yb, zb = self.c.at[u], self.xb.at[u], self.yb.at[u], self.zb.at[u]
        if stage == 0:
            self.go(u, 0, grad.at[:, :, rows, oth], c, p.core_peer)
        elif stage == 1:
            self.arrived(u, 0, c)

            def add(i, carry):
                a, b = i // 2, i % 2
                c[a, b] = (c[a, b].astype(F32) + grad[a, b, rows, own].astype(F32)).astype(BF)
                return carry

            lax.fori_loop(0, 8, add, 0)
            self.go(u, 1, c.at[:, :, :, peer_exc], xb, p.x_peer)
        elif stage == 2:
            self.arrived(u, 1, xb)

            def add(i, carry):
                a, b = i // 2, i % 2
                c[a, b, :, exc] = (c[a, b, :, exc].astype(F32) + xb[a, b].astype(F32)).astype(BF)
                return carry

            lax.fori_loop(0, 8, add, 0)
            self.go(u, 2, c.at[:, 1 - p.y, :, two], yb, p.y_peer)
        elif stage == 3:
            self.arrived(u, 2, yb)

            def add(a, carry):
                c[a, p.y, :, two] = (c[a, p.y, :, two].astype(F32) + yb[a].astype(F32)).astype(BF)
                return carry

            lax.fori_loop(0, 4, add, 0)
            for k in (1, 2, 3):
                self.go(u, 2 + k, c.at[p.z_up(k), p.y, :, two], zb.at[k - 1], p.z_peer(k))
        elif stage == 4:
            for k in (1, 2, 3):
                self.arrived(u, 2 + k, zb.at[k - 1])
            total = c[p.z, p.y, :, two].astype(F32)
            for k in (1, 2, 3):
                total = total + zb[k - 1].astype(F32)
            self.f[u, 0] = total.astype(BF)
            self.go(u, 6, self.f.at[u, 0], self.f.at[u, 1], p.x_peer)
        elif stage == 5:
            self.arrived(u, 6, self.f.at[u, 1])
            low = self.f[u, p.x].astype(F32)
            high = self.f[u, 1 - p.x].astype(F32)
            self.e[u, 0, :, 0:128] = low[:, 0:128].astype(BF)
            self.e[u, 0, :, 128:256] = (low[:, 128:] + high[:, :128]).astype(BF)
            self.e[u, 0, :, 256:384] = high[:, 128:].astype(BF)
            self.go(u, 7, self.e.at[u, 0], self.e.at[u, 1], p.core_peer)
        else:
            self.arrived(u, 7, self.e.at[u, 1])
            out = self.outs[name]
            out[rows, own] = self.e[u, 0].astype(F32)
            out[rows, oth] = self.e[u, 1].astype(F32)

    def small_stage(self, stage, mine=None):
        p, s = self.p, self.s
        peers = [p.core_peer, p.x_peer, p.y_peer]
        if stage == 0:
            s[0] = mine
        elif stage <= 3:
            i = stage - 1
            dst = s.at[2 * i + 1]
            remote(dst, dst, self.ssend.at[i], self.srecv.at[i], p.x_peer).wait_recv()
            s[2 * i + 2] = s[2 * i] + s[2 * i + 1]
        if stage < 3:
            copy = remote(s.at[2 * stage], s.at[2 * stage + 1], self.ssend.at[stage], self.srecv.at[stage], peers[stage])
            copy.start()
            self.sent.append(copy)
        elif stage == 3:
            for k in (1, 2, 3):
                copy = remote(s.at[6], s.at[6 + k], self.ssend.at[2 + k], self.srecv.at[2 + k], p.z_peer(k))
                copy.start()
                self.sent.append(copy)
        else:
            total = s[6]
            for k in (1, 2, 3):
                dst = s.at[6 + k]
                remote(dst, dst, self.ssend.at[2 + k], self.srecv.at[2 + k], p.x_peer).wait_recv()
                total = total + s[6 + k]
            return total

    def finish(self):
        for copy in self.sent:
            copy.wait_send()


def kernel_params(cid, side=True):
    return pltpu.CompilerParams(collective_id=cid, has_side_effects=side, vmem_limit_bytes=64 << 20)


VM = pl.BlockSpec(memory_space=pltpu.VMEM)
ANY = pl.BlockSpec(memory_space=pl.ANY)
NAMES = ("qkv", "out", "fc1", "fc2")
FULL = {"qkv": (4, 2, 96, 2304), "out": (4, 2, 96, 768), "fc1": (4, 2, 96, 3072), "fc2": (4, 2, 384, 768)}


def gather_kernel(*refs):
    shards = dict(zip(NAMES, refs[0:4]))
    small = refs[4]
    full = dict(zip(NAMES, refs[5:9]))
    small_full = refs[9]
    g = None
    place = Place()
    place.greet()
    g = Gather(place, shards, full, small, small_full, *refs[10:])
    for st in range(3):
        g.small_stage(st) if st == 0 else None
    for t in range(NU + 4):
        for st in (4, 3, 2, 1, 0):
            u = t - st
            if 0 <= u < NU:
                g.stage(u, st)
        if t == 1:
            g.small_stage(1)
        if t == 2:
            g.small_stage(2)
    g.finish()


def gather_call(qkv, out, fc1, fc2, small):
    return pl.pallas_call(
        gather_kernel,
        out_shape=[jax.ShapeDtypeStruct(FULL[k], BF) for k in NAMES] + [jax.ShapeDtypeStruct((4, 2, 16, 128), BF)],
        in_specs=[VM] * 5,
        out_specs=[VM] * 5,
        scratch_shapes=Gather.SEMS,
        compiler_params=kernel_params(0),
        name="gather",
    )(qkv, out, fc1, fc2, small)


def reduce_kernel(*refs):
    grads = dict(zip(NAMES, refs[0:4]))
    small = refs[4]
    outs = dict(zip(NAMES, refs[5:9]))
    small_out = refs[9]
    place = Place()
    place.greet()
    r = Reduce(place, grads, outs, refs[10:])
    r.small_stage(0, small[...])
    for t in range(NU + 6):
        for st in (6, 5, 4, 3, 2, 1, 0):
            u = t - st
            if 0 <= u < NU:
                r.stage(u, st)
        if 1 <= t <= 3:
            r.small_stage(t)
        if t == 4:
            small_out[...] = r.small_stage(4)
    r.finish()


SHARD = {"qkv": (96, 2304), "out": (96, 768), "fc1": (96, 3072), "fc2": (384, 768)}


def reduce_call(qkv, out, fc1, fc2, small):
    return pl.pallas_call(
        reduce_kernel,
        out_shape=[jax.ShapeDtypeStruct(SHARD[k], F32) for k in NAMES] + [jax.ShapeDtypeStruct((16, 768), F32)],
        in_specs=[VM] * 5,
        out_specs=[VM] * 5,
        scratch_shapes=Reduce.SCRATCH,
        compiler_params=kernel_params(1),
        name="reduce",
    )(qkv, out, fc1, fc2, small)


def compute(patches, cotangent, mask_index, mask_count, gathered):
    (
        embed_full,
        gain_attn,
        shift_attn,
        weight_qkv,
        query_bias,
        value_bias,
        weight_out,
        out_bias,
        gain_mlp,
        shift_mlp,
        weight_fc1,
        fc1_bias,
        weight_fc2,
        fc2_bias,
    ) = gathered
    clip_count, seq_len, feature_count = patches.shape
    row_count = clip_count * seq_len
    slot_ids = lax.broadcasted_iota(jnp.int32, (1, mask_index.shape[1]), 1)
    valid_slots = (slot_ids < mask_count[:, None]).astype(jnp.float32)
    patch_ids = lax.broadcasted_iota(jnp.int32, (1, 1, seq_len), 2)
    onehot = (mask_index[:, :, None] == patch_ids).astype(jnp.float32)
    masked = jnp.einsum("cj,cjp->cp", valid_slots, onehot).reshape(row_count, 1)
    kept_rows = 1.0 - masked
    start_rows = (
        patches.reshape(row_count, feature_count).astype(jnp.float32) * kept_rows
        + masked * embed_full.astype(jnp.float32)[None, :]
    )
    normed_attn, rstd_attn = norm_rows(start_rows)
    attn_in = (
        normed_attn * gain_attn.astype(jnp.float32)[None, :]
        + shift_attn.astype(jnp.float32)[None, :]
    ).astype(jnp.bfloat16)
    qkv_bias = jnp.concatenate([query_bias, jnp.zeros_like(query_bias), value_bias]).astype(
        jnp.float32
    )
    qkv = (
        jnp.dot(attn_in, weight_qkv, preferred_element_type=jnp.float32) + qkv_bias[None, :]
    ).astype(jnp.bfloat16)
    qkv_clips = qkv.reshape(clip_count, seq_len, 3 * feature_count)
    attn_mixed, log_total = lax.map(attend, qkv_clips)
    attn_mixed = attn_mixed.reshape(row_count, feature_count)
    middle = start_rows + (
        jnp.dot(attn_mixed, weight_out, preferred_element_type=jnp.float32)
        + out_bias.astype(jnp.float32)[None, :]
    )
    normed_mlp, rstd_mlp = norm_rows(middle)
    mlp_in = (
        normed_mlp * gain_mlp.astype(jnp.float32)[None, :] + shift_mlp.astype(jnp.float32)[None, :]
    ).astype(jnp.bfloat16)
    hidden = (
        jnp.dot(mlp_in, weight_fc1, preferred_element_type=jnp.float32)
        + fc1_bias.astype(jnp.float32)[None, :]
    )
    activated = jax.nn.gelu(hidden, approximate=False).astype(jnp.bfloat16)
    result = middle + (
        jnp.dot(activated, weight_fc2, preferred_element_type=jnp.float32)
        + fc2_bias.astype(jnp.float32)[None, :]
    )
    output = result.astype(jnp.bfloat16).reshape(clip_count, seq_len, feature_count)
    grad_result = cotangent.reshape(row_count, feature_count)
    grad_w_fc2 = dot_rows(activated, grad_result)
    grad_bias_fc2 = jnp.sum(grad_result.astype(jnp.float32), axis=0)
    grad_act = dot_back(grad_result, weight_fc2)
    gelu_slope = (
        0.5 * (1.0 + lax.erf(hidden * inv_root_two))
        + hidden * jnp.exp(-0.5 * hidden * hidden) * inv_root_tau
    )
    grad_hidden = (grad_act * gelu_slope).astype(jnp.bfloat16)
    grad_w_fc1 = dot_rows(mlp_in, grad_hidden)
    grad_bias_fc1 = jnp.sum(grad_hidden.astype(jnp.float32), axis=0)
    grad_mlp_in = dot_back(grad_hidden, weight_fc1)
    grad_ln2_gain = jnp.sum(grad_mlp_in * normed_mlp, axis=0)
    grad_ln2_bias = jnp.sum(grad_mlp_in, axis=0)
    grad_middle = grad_result.astype(jnp.float32) + norm_back(
        grad_mlp_in, normed_mlp, rstd_mlp, gain_mlp.astype(jnp.float32)
    )
    grad_branch = grad_middle.astype(jnp.bfloat16)
    grad_w_out = dot_rows(attn_mixed, grad_branch)
    grad_bias_out = jnp.sum(grad_branch.astype(jnp.float32), axis=0)
    grad_mixed = dot_back(grad_branch, weight_out).astype(jnp.bfloat16)
    grad_qkv = lax.map(
        attend_back, (qkv_clips, grad_mixed.reshape(clip_count, seq_len, feature_count), log_total)
    )
    grad_qkv = grad_qkv.reshape(row_count, 3 * feature_count)
    grad_w_qkv = dot_rows(attn_in, grad_qkv)
    qkv_sums = jnp.sum(grad_qkv.astype(jnp.float32), axis=0)
    grad_bias_q = qkv_sums[:feature_count]
    grad_bias_v = qkv_sums[2 * feature_count :]
    grad_attn_in = dot_back(grad_qkv, weight_qkv)
    grad_ln1_gain = jnp.sum(grad_attn_in * normed_attn, axis=0)
    grad_ln1_bias = jnp.sum(grad_attn_in, axis=0)
    grad_start = grad_middle + norm_back(
        grad_attn_in, normed_attn, rstd_attn, gain_attn.astype(jnp.float32)
    )
    grad_mask_embed = jnp.sum(grad_start * masked, axis=0)
    patch_grad = (
        (grad_start * kept_rows).astype(jnp.bfloat16).reshape(clip_count, seq_len, feature_count)
    )
    return output, patch_grad, (
        grad_mask_embed,
        grad_ln1_gain,
        grad_ln1_bias,
        grad_w_qkv,
        grad_bias_q,
        grad_bias_v,
        grad_w_out,
        grad_bias_out,
        grad_ln2_gain,
        grad_ln2_bias,
        grad_w_fc1,
        grad_bias_fc1,
        grad_w_fc2,
        grad_bias_fc2,
    )


def plain_gather(shards):
    return tuple(lax.all_gather(s, "wide", axis=0, tiled=True) for s in shards)


def plain_reduce(grads):
    shards = [lax.psum_scatter(g, "wide", scatter_dimension=0, tiled=True) for g in grads]
    return tuple(lax.psum(s.astype(BF), "narrow").astype(F32) for s in shards)


SMALL = (0, 1, 2, 4, 5, 7, 8, 9, 13)
BIG = (3, 6, 10, 12)


def kernel_gather(shards):
    rows = jnp.stack([shards[i] for i in SMALL] + list(shards[11].reshape(4, 96)))
    small = jnp.pad(rows, ((0, 3), (0, 32)))
    *full, small_full = gather_call(*[shards[i] for i in BIG], small)
    small_full = small_full.reshape(8, 16, 128)[:, :, :96]
    vectors = small_full[:, :9].transpose(1, 0, 2).reshape(9, 768)
    result = [None] * 14
    for i, row in zip(SMALL, range(9)):
        result[i] = vectors[row]
    for i, block in zip(BIG, full):
        result[i] = block.reshape(-1, block.shape[3])
    result[11] = small_full[:, 9:13].reshape(3072)
    return tuple(result)


def kernel_reduce(grads):
    small = jnp.concatenate(
        [jnp.stack([grads[i] for i in SMALL]), grads[11].reshape(4, 768), jnp.zeros((3, 768), F32)]
    )
    blocks = [grads[i].astype(BF).reshape(FULL[k]) for i, k in zip(BIG, NAMES)]
    *outs, total = reduce_call(*blocks, small)
    place = lax.axis_index("wide")
    mine = lax.dynamic_slice(total, (0, place * 96), (9, 96))
    result = [None] * 14
    for i, row in zip(SMALL, range(9)):
        result[i] = mine[row]
    for i, block in zip(BIG, outs):
        result[i] = block
    result[11] = lax.dynamic_slice(total[9:13].reshape(3072), (place * 384,), (384,))
    return tuple(result)


def per_device(kernels, patches, cotangent, mask_index, mask_count, *shards):
    gathered = (kernel_gather if kernels else plain_gather)(shards)
    output, patch_grad, grads = compute(patches, cotangent, mask_index, mask_count, gathered)
    return (output, patch_grad) + (kernel_reduce if kernels else plain_reduce)(grads)


def solution(mesh):
    in_specs = (
        P(("narrow", "wide"), None, None),
        P(("narrow", "wide"), None, None),
        P(("narrow", "wide"), None),
        P(("narrow", "wide")),
        P("wide"),
        P("wide"),
        P("wide"),
        P("wide", None),
        P("wide"),
        P("wide"),
        P("wide", None),
        P("wide"),
        P("wide"),
        P("wide"),
        P("wide", None),
        P("wide"),
        P("wide", None),
        P("wide"),
    )
    out_specs = (
        P(("narrow", "wide"), None, None),
        P(("narrow", "wide"), None, None),
        P("wide"),
        P("wide"),
        P("wide"),
        P("wide", None),
        P("wide"),
        P("wide"),
        P("wide", None),
        P("wide"),
        P("wide"),
        P("wide"),
        P("wide", None),
        P("wide"),
        P("wide", None),
        P("wide"),
    )
    kernels = mesh.shape["narrow"] == 4 and mesh.shape["wide"] == 8
    return jax.shard_map(
        functools.partial(per_device, kernels), mesh=mesh, in_specs=in_specs, out_specs=out_specs, check_vma=False
    )
```

```python
import jax
import jax.numpy as jnp
from jax import lax
from jax.experimental import pallas as pl
from jax.experimental.pallas import tpu as pltpu
from jax.sharding import PartitionSpec as P

HEADS = 12
HD = 64


epsilon = 1e-06
inv_root_two = 0.7071067811865476
inv_root_tau = 0.3989422804014327


def dot_rows(left_side, right_side):
    return lax.dot_general(
        left_side, right_side, (((0,), (0,)), ((), ())), preferred_element_type=jnp.float32
    )


def dot_back(left_side, right_side):
    return lax.dot_general(
        left_side, right_side, (((1,), (1,)), ((), ())), preferred_element_type=jnp.float32
    )


def norm_rows(values):
    row_mean = jnp.mean(values, axis=-1, keepdims=True)
    centered = values - row_mean
    variance = jnp.mean(centered * centered, axis=-1, keepdims=True)
    inv_std = lax.rsqrt(variance + epsilon)
    return (centered * inv_std, inv_std)


def norm_back(grad_in, normed, inv_std, ln_gain):
    grad_normed = grad_in * ln_gain[None, :]
    mean_grad = jnp.mean(grad_normed, axis=-1, keepdims=True)
    mean_cross = jnp.mean(grad_normed * normed, axis=-1, keepdims=True)
    return inv_std * (grad_normed - mean_grad - normed * mean_cross)


def split_heads(qkv_clip):
    seq_len = qkv_clip.shape[0]
    split_qkv = qkv_clip.reshape(seq_len, 3, HEADS, HD)
    return (split_qkv[:, 0], split_qkv[:, 1], split_qkv[:, 2])


def clip_scores(query_rows, key_rows):
    return jnp.einsum(
        "qhd,khd->hqk", query_rows, key_rows, preferred_element_type=jnp.float32
    ) * HD ** (-0.5)


def attend(qkv_clip):
    query_rows, key_rows, value_rows = split_heads(qkv_clip)
    scores = clip_scores(query_rows, key_rows)
    row_max = jnp.max(scores, axis=-1, keepdims=True)
    exp_scores = jnp.exp(scores - row_max)
    row_total = jnp.sum(exp_scores, axis=-1, keepdims=True)
    soft_probs = (exp_scores / row_total).astype(jnp.bfloat16)
    attn_mixed = jnp.einsum(
        "hqk,khd->qhd", soft_probs, value_rows, preferred_element_type=jnp.float32
    )
    log_total = (row_max + jnp.log(row_total))[..., 0]
    return (attn_mixed.reshape(qkv_clip.shape[0], HEADS * HD).astype(jnp.bfloat16), log_total)


def attend_back(block_args):
    qkv_clip, grad_mixed, log_total = block_args
    query_rows, key_rows, value_rows = split_heads(qkv_clip)
    grad_heads = grad_mixed.reshape(qkv_clip.shape[0], HEADS, HD)
    soft_probs = jnp.exp(clip_scores(query_rows, key_rows) - log_total[..., None])
    grad_probs = jnp.einsum(
        "qhd,khd->hqk", grad_heads, value_rows, preferred_element_type=jnp.float32
    )
    grad_value = jnp.einsum(
        "hqk,qhd->khd",
        soft_probs.astype(jnp.bfloat16),
        grad_heads,
        preferred_element_type=jnp.float32,
    )
    grad_scores = soft_probs * (
        grad_probs - jnp.sum(soft_probs * grad_probs, axis=-1, keepdims=True)
    )
    grad_scores = grad_scores.astype(jnp.bfloat16)
    grad_query = jnp.einsum(
        "hqk,khd->qhd", grad_scores, key_rows, preferred_element_type=jnp.float32
    ) * HD ** (-0.5)
    grad_key = jnp.einsum(
        "hqk,qhd->khd", grad_scores, query_rows, preferred_element_type=jnp.float32
    ) * HD ** (-0.5)
    stacked = jnp.stack([grad_query, grad_key, grad_value], axis=1)
    return stacked.reshape(qkv_clip.shape[0], 3 * HEADS * HD).astype(jnp.bfloat16)


MESH = pl.DeviceIdType.MESH
BF = jnp.bfloat16
F32 = jnp.float32

UNITS = (
    [("qkv", 768 * j, 0) for j in range(3)]
    + [("out", 0, 0)]
    + [("fc1", 768 * j, 0) for j in range(4)]
    + [("fc2", 0, 96 * j) for j in range(4)]
)
NU = len(UNITS)


def lanes(start):
    return pl.multiple_of(start, 128)


class Place:
    def __init__(self):
        n = lax.axis_index("narrow")
        w = lax.axis_index("wide")
        self.n, self.w = n, w
        self.core, self.x = n % 2, n // 2
        self.y, self.z = w % 2, w // 2
        self.core_peer = (self.x * 2 + (1 - self.core), w)
        self.x_peer = ((1 - self.x) * 2 + self.core, w)
        self.y_peer = (n, self.z * 2 + (1 - self.y))

    def z_up(self, k):
        return (self.z + k) % 4

    def z_peer(self, k):
        return (self.n, self.z_up(k) * 2 + self.y)

    def greet(self):
        barrier = pltpu.get_barrier_semaphore()
        peers = [self.core_peer, self.x_peer, self.y_peer] + [self.z_peer(k) for k in (1, 2, 3)]
        for peer in peers:
            pl.semaphore_signal(barrier, inc=1, device_id=peer, device_id_type=MESH)
        pl.semaphore_wait(barrier, len(peers))


def remote(src, dst, send, recv, peer):
    return pltpu.make_async_remote_copy(
        src_ref=src, dst_ref=dst, send_sem=send, recv_sem=recv, device_id=peer, device_id_type=MESH
    )


class Gather:
    SEMS = [
        pltpu.SemaphoreType.DMA((NU, 10)),
        pltpu.SemaphoreType.DMA((NU, 10)),
        pltpu.SemaphoreType.DMA((NU,)),
        pltpu.SemaphoreType.DMA((8,)),
        pltpu.SemaphoreType.DMA((8,)),
    ]

    def __init__(self, place, shards, full, small, small_full, send, recv, local, ssend, srecv):
        self.p, self.shards, self.full = place, shards, full
        self.small, self.small_full = small, small_full
        self.send, self.recv, self.local, self.ssend, self.srecv = send, recv, local, ssend, srecv
        self.sent = []

    def go(self, u, i, src, dst, peer):
        copy = remote(src, dst, self.send.at[u, i], self.recv.at[u, i], peer)
        copy.start()
        self.sent.append(copy)

    def arrived(self, u, i, dst):
        remote(dst, dst, self.send.at[u, i], self.recv.at[u, i], self.p.x_peer).wait_recv()

    def small_stage(self, stage):
        p = self.p
        if stage == 0:
            own = self.small_full.at[p.z, p.y]
            pltpu.make_async_copy(self.small, own, self.local.at[0]).start()
            pltpu.make_async_copy(self.small, own, self.local.at[0]).wait()
            for k in (1, 2, 3):
                copy = remote(self.small, own, self.ssend.at[k], self.srecv.at[k], p.z_peer(k))
                copy.start()
                self.sent.append(copy)
        elif stage == 1:
            for k in (1, 2, 3):
                dst = self.small_full.at[p.z_up(4 - k), p.y]
                remote(dst, dst, self.ssend.at[k], self.srecv.at[k], p.x_peer).wait_recv()
            mine = self.small_full.at[:, p.y]
            copy = remote(mine, mine, self.ssend.at[0], self.srecv.at[0], p.y_peer)
            copy.start()
            self.sent.append(copy)
        else:
            dst = self.small_full.at[:, 1 - p.y]
            remote(dst, dst, self.ssend.at[0], self.srecv.at[0], p.x_peer).wait_recv()

    def stage(self, u, stage):
        p = self.p
        name, co, ro = UNITS[u]
        full, shard = self.full[name], self.shards[name]
        rows = pl.ds(ro, 96)
        own = pl.ds(lanes(co + p.core * 384 + p.x * 128), 256)
        exc = pl.ds(lanes(co + p.core * 384 + p.x * 256), 128)
        peer_exc = pl.ds(lanes(co + p.core * 384 + (1 - p.x) * 256), 128)
        oth = pl.ds(lanes(co + (1 - p.core) * 384 + p.x * 128), 256)
        oth_exc = pl.ds(lanes(co + (1 - p.core) * 384 + (1 - p.x) * 256), 128)
        if stage == 0:
            mine = shard.at[rows, own]
            home = full.at[p.z, p.y, rows, own]
            pltpu.make_async_copy(mine, home, self.local.at[u]).start()
            for k in (1, 2, 3):
                self.go(u, k, mine, home, p.z_peer(k))
        elif stage == 1:
            home = full.at[p.z, p.y, rows, own]
            pltpu.make_async_copy(shard.at[rows, own], home, self.local.at[u]).wait()
            for k in (1, 2, 3):
                self.arrived(u, k, full.at[p.z_up(4 - k), p.y, rows, own])
            column = full.at[:, p.y, rows, own]
            part = full.at[:, p.y, rows, exc]
            self.go(u, 0, column, column, p.y_peer)
            self.go(u, 4, part, part, p.x_peer)
            self.go(u, 5, column, column, p.core_peer)
        elif stage == 2:
            column = full.at[:, 1 - p.y, rows, own]
            part = full.at[:, 1 - p.y, rows, exc]
            self.arrived(u, 0, column)
            self.go(u, 6, part, part, p.x_peer)
            self.go(u, 7, column, column, p.core_peer)
        elif stage == 3:
            self.arrived(u, 4, full.at[:, p.y, rows, peer_exc])
            self.arrived(u, 6, full.at[:, 1 - p.y, rows, peer_exc])
            both = full.at[:, :, rows, peer_exc]
            self.go(u, 8, both, both, p.core_peer)
        else:
            self.arrived(u, 5, full.at[:, p.y, rows, oth])
            self.arrived(u, 7, full.at[:, 1 - p.y, rows, oth])
            self.arrived(u, 8, full.at[:, :, rows, oth_exc])

    def finish(self):
        for copy in self.sent:
            copy.wait_send()


class Reduce:
    SCRATCH = [
        pltpu.VMEM((NU, 4, 2, 96, 384), BF),
        pltpu.VMEM((NU, 4, 2, 96, 128), BF),
        pltpu.VMEM((NU, 4, 96, 256), BF),
        pltpu.VMEM((NU, 3, 96, 256), BF),
        pltpu.VMEM((NU, 2, 96, 256), BF),
        pltpu.VMEM((NU, 2, 96, 384), BF),
        pltpu.VMEM((10, 16, 768), F32),
        pltpu.SemaphoreType.DMA((NU, 8)),
        pltpu.SemaphoreType.DMA((NU, 8)),
        pltpu.SemaphoreType.DMA((6,)),
        pltpu.SemaphoreType.DMA((6,)),
    ]

    def __init__(self, place, grads, outs, bufs):
        self.p, self.grads, self.outs = place, grads, outs
        (self.c, self.xb, self.yb, self.zb, self.f, self.e, self.s,
         self.send, self.recv, self.ssend, self.srecv) = bufs
        self.sent = []

    def go(self, u, i, src, dst, peer):
        copy = remote(src, dst, self.send.at[u, i], self.recv.at[u, i], peer)
        copy.start()
        self.sent.append(copy)

    def arrived(self, u, i, dst):
        remote(dst, dst, self.send.at[u, i], self.recv.at[u, i], self.p.x_peer).wait_recv()

    def stage(self, u, stage):
        p = self.p
        name, co, ro = UNITS[u]
        grad = self.grads[name]
        rows = pl.ds(ro, 96)
        own = pl.ds(lanes(co + p.core * 384), 384)
        oth = pl.ds(lanes(co + (1 - p.core) * 384), 384)
        exc = pl.ds(lanes(p.x * 256), 128)
        peer_exc = pl.ds(lanes((1 - p.x) * 256), 128)
        two = pl.ds(lanes(p.x * 128), 256)
        c, xb, yb, zb = self.c.at[u], self.xb.at[u], self.yb.at[u], self.zb.at[u]
        if stage == 0:
            self.go(u, 0, grad.at[:, :, rows, oth], c, p.core_peer)
        elif stage == 1:
            self.arrived(u, 0, c)

            def add(i, carry):
                a, b = i // 2, i % 2
                c[a, b] = (c[a, b].astype(F32) + grad[a, b, rows, own].astype(F32)).astype(BF)
                return carry

            lax.fori_loop(0, 8, add, 0)
            self.go(u, 1, c.at[:, :, :, peer_exc], xb, p.x_peer)
        elif stage == 2:
            self.arrived(u, 1, xb)

            def add(i, carry):
                a, b = i // 2, i % 2
                c[a, b, :, exc] = (c[a, b, :, exc].astype(F32) + xb[a, b].astype(F32)).astype(BF)
                return carry

            lax.fori_loop(0, 8, add, 0)
            self.go(u, 2, c.at[:, 1 - p.y, :, two], yb, p.y_peer)
        elif stage == 3:
            self.arrived(u, 2, yb)

            def add(a, carry):
                c[a, p.y, :, two] = (c[a, p.y, :, two].astype(F32) + yb[a].astype(F32)).astype(BF)
                return carry

            lax.fori_loop(0, 4, add, 0)
            for k in (1, 2, 3):
                self.go(u, 2 + k, c.at[p.z_up(k), p.y, :, two], zb.at[k - 1], p.z_peer(k))
        elif stage == 4:
            for k in (1, 2, 3):
                self.arrived(u, 2 + k, zb.at[k - 1])
            total = c[p.z, p.y, :, two].astype(F32)
            for k in (1, 2, 3):
                total = total + zb[k - 1].astype(F32)
            self.f[u, 0] = total.astype(BF)
            self.go(u, 6, self.f.at[u, 0], self.f.at[u, 1], p.x_peer)
        elif stage == 5:
            self.arrived(u, 6, self.f.at[u, 1])
            low = self.f[u, p.x].astype(F32)
            high = self.f[u, 1 - p.x].astype(F32)
            self.e[u, 0, :, 0:128] = low[:, 0:128].astype(BF)
            self.e[u, 0, :, 128:256] = (low[:, 128:] + high[:, :128]).astype(BF)
            self.e[u, 0, :, 256:384] = high[:, 128:].astype(BF)
            self.go(u, 7, self.e.at[u, 0], self.e.at[u, 1], p.core_peer)
        else:
            self.arrived(u, 7, self.e.at[u, 1])
            out = self.outs[name]
            out[rows, own] = self.e[u, 0].astype(F32)
            out[rows, oth] = self.e[u, 1].astype(F32)

    def small_stage(self, stage, mine=None):
        p, s = self.p, self.s
        peers = [p.core_peer, p.x_peer, p.y_peer]
        if stage == 0:
            s[0] = mine
        elif stage <= 3:
            i = stage - 1
            dst = s.at[2 * i + 1]
            remote(dst, dst, self.ssend.at[i], self.srecv.at[i], p.x_peer).wait_recv()
            s[2 * i + 2] = s[2 * i] + s[2 * i + 1]
        if stage < 3:
            copy = remote(s.at[2 * stage], s.at[2 * stage + 1], self.ssend.at[stage], self.srecv.at[stage], peers[stage])
            copy.start()
            self.sent.append(copy)
        elif stage == 3:
            for k in (1, 2, 3):
                copy = remote(s.at[6], s.at[6 + k], self.ssend.at[2 + k], self.srecv.at[2 + k], p.z_peer(k))
                copy.start()
                self.sent.append(copy)
        else:
            total = s[6]
            for k in (1, 2, 3):
                dst = s.at[6 + k]
                remote(dst, dst, self.ssend.at[2 + k], self.srecv.at[2 + k], p.x_peer).wait_recv()
                total = total + s[6 + k]
            return total

    def finish(self):
        for copy in self.sent:
            copy.wait_send()


def kernel_params(cid, side=True):
    return pltpu.CompilerParams(collective_id=cid, has_side_effects=side, vmem_limit_bytes=67043328)


VM = pl.BlockSpec(memory_space=pltpu.VMEM)
ANY = pl.BlockSpec(memory_space=pl.ANY)
NAMES = ("qkv", "out", "fc1", "fc2")
FULL = {"qkv": (4, 2, 96, 2304), "out": (4, 2, 96, 768), "fc1": (4, 2, 96, 3072), "fc2": (4, 2, 384, 768)}


def reduce_kernel(*refs):
    grads = dict(zip(NAMES, refs[0:4]))
    small = refs[4]
    outs = dict(zip(NAMES, refs[5:9]))
    small_out = refs[9]
    place = Place()
    place.greet()
    r = Reduce(place, grads, outs, refs[10:])
    r.small_stage(0, small[...])
    for t in range(NU + 6):
        for st in range(7):
            u = t - st
            if 0 <= u < NU:
                r.stage(u, st)
        if 1 <= t <= 3:
            r.small_stage(t)
        if t == 4:
            small_out[...] = r.small_stage(4)
    r.finish()


SHARD = {"qkv": (96, 2304), "out": (96, 768), "fc1": (96, 3072), "fc2": (384, 768)}


def reduce_call(qkv, out, fc1, fc2, small):
    return pl.pallas_call(
        reduce_kernel,
        out_shape=[jax.ShapeDtypeStruct(SHARD[k], F32) for k in NAMES] + [jax.ShapeDtypeStruct((16, 768), F32)],
        in_specs=[VM] * 5,
        out_specs=[VM] * 5,
        scratch_shapes=Reduce.SCRATCH,
        compiler_params=kernel_params(1),
        name="reduce",
    )(qkv, out, fc1, fc2, small)

def row_block(i, size):
    return pl.ds(pl.multiple_of(i * size, size), size)


class Ticks:
    def __init__(self, run, stages, ahead):
        self.run, self.stages, self.ahead = run, stages, ahead
        self.t = 0
        for u in range(ahead):
            run(u, 0)

    def tick(self):
        t = self.t
        self.t += 1
        if t + self.ahead < NU:
            self.run(t + self.ahead, 0)
        for s in range(1, self.stages):
            if 0 <= t - s + 1 < NU:
                self.run(t - s + 1, s)

    def need(self, u):
        while self.t < u + self.stages - 1:
            self.tick()


def matmul(left, right):
    return jnp.dot(left, right, preferred_element_type=F32)


def norm_block(values):
    mean = jnp.mean(values, axis=1, keepdims=True)
    centered = values - mean
    variance = jnp.mean(centered * centered, axis=1, keepdims=True)
    inv_std = lax.rsqrt(variance + epsilon)
    return centered * inv_std, inv_std


KEPT = (
    ("attn_in", (1024, 768), BF),
    ("normed1", (1024, 768), BF),
    ("rstd1", (1024, 128), F32),
    ("qkv", (1024, 2304), BF),
    ("mixed", (1024, 768), BF),
    ("mlp_in", (1024, 768), BF),
    ("normed2", (1024, 768), BF),
    ("rstd2", (1024, 128), F32),
    ("act", (1024, 3072), BF),
    ("slope", (1024, 3072), BF),
    ("out", (1024, 768), BF),
    ("vec", (16, 768), F32),
)


def attend_pair(qkv, mixed, i):
    clip, pair = i // 6, i % 6
    rows = row_block(clip, 512)
    at = pl.multiple_of(pair * 128, 128)
    q2 = qkv[rows, pl.ds(at, 128)]
    k2 = qkv[rows, pl.ds(pl.multiple_of(at + 768, 128), 128)]
    v2 = qkv[rows, pl.ds(pl.multiple_of(at + 1536, 128), 128)]
    lane = lax.broadcasted_iota(jnp.int32, (512, 128), 1)
    parts = []
    for h in range(2):
        inside = (lane >= 64) if h else (lane < 64)
        qh = jnp.where(inside, q2 * jnp.asarray(0.125, BF), jnp.zeros_like(q2))
        scores = lax.dot_general(qh, k2, (((1,), (1,)), ((), ())), preferred_element_type=F32)
        e = jnp.exp(scores - jnp.max(scores, axis=1, keepdims=True))
        total = jnp.sum(e, axis=1, keepdims=True)
        parts.append(matmul(e.astype(BF), v2) * (1.0 / total))
    mixed[rows, pl.ds(at, 128)] = jnp.where(lane < 64, parts[0], parts[1]).astype(BF)


def forward_kernel(*refs):
    patches, mask = refs[0:2]
    shards = dict(zip(NAMES, refs[2:6]))
    small = refs[6]
    n_out = 4 + len(KEPT)
    full_out = dict(zip(NAMES, refs[7:11]))
    kept_out = dict(zip([k[0] for k in KEPT], refs[11 : 7 + n_out]))
    rest = refs[7 + n_out :]
    full = dict(zip(NAMES, rest[0:4]))
    kept = dict(zip([k[0] for k in KEPT], rest[4 : 4 + len(KEPT)]))
    middle, small_full, bias1, out_sem = rest[4 + len(KEPT) : 8 + len(KEPT)]
    sems = rest[8 + len(KEPT) :]
    place = Place()
    place.greet()
    g = Gather(place, shards, full, small, small_full, *sems)
    leaving = []

    def leave(src, dst):
        copy = pltpu.make_async_copy(src, dst, out_sem.at[len(leaving)])
        copy.start()
        leaving.append(copy)

    def keep(name):
        leave(kept[name], kept_out[name])

    g.small_stage(0)
    ticks = Ticks(g.stage, 5, 3)
    g.small_stage(1)
    g.small_stage(2)
    ticks.tick()
    vec = kept["vec"]
    total = jnp.zeros((16, 768), F32)
    spot = lax.broadcasted_iota(jnp.int32, (128, 768), 1) - lax.broadcasted_iota(jnp.int32, (128, 768), 0)
    inside = lax.broadcasted_iota(jnp.int32, (128, 768), 0) < 96
    for s in range(8):
        block = small_full[s // 2, s % 2]
        pick = jnp.where((spot == 96 * s) & inside, 1.0, 0.0).astype(BF)
        total = total + matmul(block, pick)
        wide = block.astype(F32)
        for r in range(3):
            bias1[:, pl.ds(s * 384 + r * 128, 128)] = jnp.broadcast_to(wide[9 + r : 10 + r, :], (8, 128))
    vec[...] = total
    keep("vec")

    def norm1(i, carry):
        rows = row_block(i, 128)
        m = mask[rows, 0:1]
        start = patches[rows, :].astype(F32) * (1.0 - m) + m * vec[0:1, :]
        normed, inv_std = norm_block(start)
        middle[rows, :] = start
        kept["normed1"][rows, :] = normed.astype(BF)
        kept["rstd1"][rows, :] = jnp.broadcast_to(inv_std, (128, 128))
        kept["attn_in"][rows, :] = (normed * vec[1:2, :] + vec[2:3, :]).astype(BF)
        return carry

    lax.fori_loop(0, 8, norm1, 0)
    for name in ("attn_in", "normed1", "rstd1"):
        keep(name)
    for u in range(3):
        ticks.need(u)
        w = full["qkv"][:, :, :, pl.ds(768 * u, 768)].reshape(768, 768)

        def project(i, carry):
            rows = row_block(i, 512)
            value = matmul(kept["attn_in"][rows, :], w)
            if u != 1:
                row = 3 if u == 0 else 4
                value = value + vec[row : row + 1, :]
            kept["qkv"][rows, pl.ds(768 * u, 768)] = value.astype(BF)
            return carry

        lax.fori_loop(0, 2, project, 0)
    leave(full["qkv"], full_out["qkv"])
    keep("qkv")
    for part in range(6):

        def attend_two(i, carry):
            attend_pair(kept["qkv"], kept["mixed"], i)
            return carry

        lax.fori_loop(2 * part, 2 * part + 2, attend_two, 0)
        ticks.tick()
    keep("mixed")
    ticks.need(3)
    leave(full["out"], full_out["out"])
    w_out = full["out"][...].reshape(768, 768)

    def mix(i, carry):
        rows = row_block(i, 512)
        middle[rows, :] = middle[rows, :] + (matmul(kept["mixed"][rows, :], w_out) + vec[5:6, :])
        return carry

    lax.fori_loop(0, 2, mix, 0)
    ticks.tick()

    def norm2(i, carry):
        rows = row_block(i, 128)
        normed, inv_std = norm_block(middle[rows, :])
        kept["normed2"][rows, :] = normed.astype(BF)
        kept["rstd2"][rows, :] = jnp.broadcast_to(inv_std, (128, 128))
        kept["mlp_in"][rows, :] = (normed * vec[6:7, :] + vec[7:8, :]).astype(BF)
        return carry

    lax.fori_loop(0, 8, norm2, 0)
    for name in ("normed2", "rstd2", "mlp_in"):
        keep(name)
    for j in range(4):
        ticks.need(4 + j)
        w = full["fc1"][:, :, :, pl.ds(768 * j, 768)].reshape(768, 768)

        def expand(i, carry):
            rows = row_block(i, 256)
            cols = pl.ds(768 * j, 768)
            h = matmul(kept["mlp_in"][rows, :], w) + bias1[0:1, cols]
            below = 0.5 * (1.0 + lax.erf(h * inv_root_two))
            density = jnp.exp(-0.5 * h * h) * inv_root_tau
            kept["act"][rows, cols] = (h * below).astype(BF)
            kept["slope"][rows, cols] = (below + h * density).astype(BF)
            return carry

        lax.fori_loop(0, 4, expand, 0)
        ticks.tick()
    leave(full["fc1"], full_out["fc1"])
    keep("act")
    keep("slope")
    ticks.need(NU - 1)
    leave(full["fc2"], full_out["fc2"])

    def contract(i, carry):
        rows = row_block(i, 512)
        value = middle[rows, :] + vec[8:9, :]
        for k in range(4):
            w = full["fc2"][k].reshape(768, 768)
            value = value + matmul(kept["act"][rows, pl.ds(768 * k, 768)], w)
        kept["out"][rows, :] = value.astype(BF)
        return carry

    lax.fori_loop(0, 2, contract, 0)
    keep("out")
    g.finish()
    for copy in leaving:
        copy.wait()


def forward_call(patches, mask, qkv, out, fc1, fc2, small):
    shapes = [jax.ShapeDtypeStruct(FULL[k], BF) for k in NAMES]
    shapes += [jax.ShapeDtypeStruct(k[1], k[2]) for k in KEPT]
    scratch = [pltpu.VMEM(FULL[k], BF) for k in NAMES]
    scratch += [pltpu.VMEM(k[1], k[2]) for k in KEPT]
    scratch += [
        pltpu.VMEM((1024, 768), F32),
        pltpu.VMEM((4, 2, 16, 128), BF),
        pltpu.VMEM((8, 3072), F32),
        pltpu.SemaphoreType.DMA((4 + len(KEPT),)),
    ]
    return pl.pallas_call(
        forward_kernel,
        out_shape=shapes,
        in_specs=[VM] * 7,
        out_specs=[ANY] * len(shapes),
        scratch_shapes=scratch + Gather.SEMS,
        compiler_params=kernel_params(0),
        name="forward",
    )(patches, mask, qkv, out, fc1, fc2, small)


def compute(patches, cotangent, mask_index, mask_count, gathered):
    (
        embed_full,
        gain_attn,
        shift_attn,
        weight_qkv,
        query_bias,
        value_bias,
        weight_out,
        out_bias,
        gain_mlp,
        shift_mlp,
        weight_fc1,
        fc1_bias,
        weight_fc2,
        fc2_bias,
    ) = gathered
    clip_count, seq_len, feature_count = patches.shape
    row_count = clip_count * seq_len
    slot_ids = lax.broadcasted_iota(jnp.int32, (1, mask_index.shape[1]), 1)
    valid_slots = (slot_ids < mask_count[:, None]).astype(jnp.float32)
    patch_ids = lax.broadcasted_iota(jnp.int32, (1, 1, seq_len), 2)
    onehot = (mask_index[:, :, None] == patch_ids).astype(jnp.float32)
    masked = jnp.einsum("cj,cjp->cp", valid_slots, onehot).reshape(row_count, 1)
    kept_rows = 1.0 - masked
    start_rows = (
        patches.reshape(row_count, feature_count).astype(jnp.float32) * kept_rows
        + masked * embed_full.astype(jnp.float32)[None, :]
    )
    normed_attn, rstd_attn = norm_rows(start_rows)
    attn_in = (
        normed_attn * gain_attn.astype(jnp.float32)[None, :]
        + shift_attn.astype(jnp.float32)[None, :]
    ).astype(jnp.bfloat16)
    qkv_bias = jnp.concatenate([query_bias, jnp.zeros_like(query_bias), value_bias]).astype(
        jnp.float32
    )
    qkv = (
        jnp.dot(attn_in, weight_qkv, preferred_element_type=jnp.float32) + qkv_bias[None, :]
    ).astype(jnp.bfloat16)
    qkv_clips = qkv.reshape(clip_count, seq_len, 3 * feature_count)
    attn_mixed, log_total = lax.map(attend, qkv_clips)
    attn_mixed = attn_mixed.reshape(row_count, feature_count)
    middle = start_rows + (
        jnp.dot(attn_mixed, weight_out, preferred_element_type=jnp.float32)
        + out_bias.astype(jnp.float32)[None, :]
    )
    normed_mlp, rstd_mlp = norm_rows(middle)
    mlp_in = (
        normed_mlp * gain_mlp.astype(jnp.float32)[None, :] + shift_mlp.astype(jnp.float32)[None, :]
    ).astype(jnp.bfloat16)
    hidden = (
        jnp.dot(mlp_in, weight_fc1, preferred_element_type=jnp.float32)
        + fc1_bias.astype(jnp.float32)[None, :]
    )
    activated = jax.nn.gelu(hidden, approximate=False).astype(jnp.bfloat16)
    result = middle + (
        jnp.dot(activated, weight_fc2, preferred_element_type=jnp.float32)
        + fc2_bias.astype(jnp.float32)[None, :]
    )
    output = result.astype(jnp.bfloat16).reshape(clip_count, seq_len, feature_count)
    grad_result = cotangent.reshape(row_count, feature_count)
    grad_w_fc2 = dot_rows(activated, grad_result)
    grad_bias_fc2 = jnp.sum(grad_result.astype(jnp.float32), axis=0)
    grad_act = dot_back(grad_result, weight_fc2)
    gelu_slope = (
        0.5 * (1.0 + lax.erf(hidden * inv_root_two))
        + hidden * jnp.exp(-0.5 * hidden * hidden) * inv_root_tau
    )
    grad_hidden = (grad_act * gelu_slope).astype(jnp.bfloat16)
    grad_w_fc1 = dot_rows(mlp_in, grad_hidden)
    grad_bias_fc1 = jnp.sum(grad_hidden.astype(jnp.float32), axis=0)
    grad_mlp_in = dot_back(grad_hidden, weight_fc1)
    grad_ln2_gain = jnp.sum(grad_mlp_in * normed_mlp, axis=0)
    grad_ln2_bias = jnp.sum(grad_mlp_in, axis=0)
    grad_middle = grad_result.astype(jnp.float32) + norm_back(
        grad_mlp_in, normed_mlp, rstd_mlp, gain_mlp.astype(jnp.float32)
    )
    grad_branch = grad_middle.astype(jnp.bfloat16)
    grad_w_out = dot_rows(attn_mixed, grad_branch)
    grad_bias_out = jnp.sum(grad_branch.astype(jnp.float32), axis=0)
    grad_mixed = dot_back(grad_branch, weight_out).astype(jnp.bfloat16)
    grad_qkv = lax.map(
        attend_back, (qkv_clips, grad_mixed.reshape(clip_count, seq_len, feature_count), log_total)
    )
    grad_qkv = grad_qkv.reshape(row_count, 3 * feature_count)
    grad_w_qkv = dot_rows(attn_in, grad_qkv)
    qkv_sums = jnp.sum(grad_qkv.astype(jnp.float32), axis=0)
    grad_bias_q = qkv_sums[:feature_count]
    grad_bias_v = qkv_sums[2 * feature_count :]
    grad_attn_in = dot_back(grad_qkv, weight_qkv)
    grad_ln1_gain = jnp.sum(grad_attn_in * normed_attn, axis=0)
    grad_ln1_bias = jnp.sum(grad_attn_in, axis=0)
    grad_start = grad_middle + norm_back(
        grad_attn_in, normed_attn, rstd_attn, gain_attn.astype(jnp.float32)
    )
    grad_mask_embed = jnp.sum(grad_start * masked, axis=0)
    patch_grad = (
        (grad_start * kept_rows).astype(jnp.bfloat16).reshape(clip_count, seq_len, feature_count)
    )
    return output, patch_grad, (
        grad_mask_embed,
        grad_ln1_gain,
        grad_ln1_bias,
        grad_w_qkv,
        grad_bias_q,
        grad_bias_v,
        grad_w_out,
        grad_bias_out,
        grad_ln2_gain,
        grad_ln2_bias,
        grad_w_fc1,
        grad_bias_fc1,
        grad_w_fc2,
        grad_bias_fc2,
    )


def plain_gather(shards):
    return tuple(lax.all_gather(s, "wide", axis=0, tiled=True) for s in shards)


def plain_reduce(grads):
    shards = [lax.psum_scatter(g, "wide", scatter_dimension=0, tiled=True) for g in grads]
    return tuple(lax.psum(s.astype(BF), "narrow").astype(F32) for s in shards)


SMALL = (0, 1, 2, 4, 5, 7, 8, 9, 13)
BIG = (3, 6, 10, 12)


def kernel_reduce(grads):
    small = jnp.concatenate(
        [jnp.stack([grads[i] for i in SMALL]), grads[11].reshape(4, 768), jnp.zeros((3, 768), F32)]
    )
    blocks = [grads[i].astype(BF).reshape(FULL[k]) for i, k in zip(BIG, NAMES)]
    *outs, total = reduce_call(*blocks, small)
    place = lax.axis_index("wide")
    mine = lax.dynamic_slice(total, (0, place * 96), (9, 96))
    result = [None] * 14
    for i, row in zip(SMALL, range(9)):
        result[i] = mine[row]
    for i, block in zip(BIG, outs):
        result[i] = block
    result[11] = lax.dynamic_slice(total[9:13].reshape(3072), (place * 384,), (384,))
    return tuple(result)


def attend_again(block_args):
    qkv_clip, grad_mixed = block_args
    query_rows, key_rows, _ = split_heads(qkv_clip)
    log_total = jax.nn.logsumexp(clip_scores(query_rows, key_rows), axis=-1)
    return attend_back((qkv_clip, grad_mixed, log_total))


def backward(cotangent, masked, full, kept):
    weight_qkv, weight_out, weight_fc1, weight_fc2 = [b.reshape(-1, b.shape[3]) for b in full]
    (attn_in, normed1, rstd1, qkv, mixed, mlp_in, normed2, rstd2, act, slope, _, vec) = kept
    normed1, normed2 = normed1.astype(F32), normed2.astype(F32)
    grad_result = cotangent.reshape(1024, 768)
    grad_w_fc2 = dot_rows(act, grad_result)
    grad_bias_fc2 = jnp.sum(grad_result.astype(F32), axis=0)
    grad_hidden = (dot_back(grad_result, weight_fc2) * slope).astype(BF)
    grad_w_fc1 = dot_rows(mlp_in, grad_hidden)
    grad_bias_fc1 = jnp.sum(grad_hidden.astype(F32), axis=0)
    grad_mlp_in = dot_back(grad_hidden, weight_fc1)
    grad_ln2_gain = jnp.sum(grad_mlp_in * normed2, axis=0)
    grad_ln2_bias = jnp.sum(grad_mlp_in, axis=0)
    grad_middle = grad_result.astype(F32) + norm_back(grad_mlp_in, normed2, rstd2[:, :1], vec[6])
    grad_branch = grad_middle.astype(BF)
    grad_w_out = dot_rows(mixed, grad_branch)
    grad_bias_out = jnp.sum(grad_branch.astype(F32), axis=0)
    grad_mixed = dot_back(grad_branch, weight_out).astype(BF)
    grad_qkv = lax.map(attend_again, (qkv.reshape(2, 512, 2304), grad_mixed.reshape(2, 512, 768)))
    grad_qkv = grad_qkv.reshape(1024, 2304)
    grad_w_qkv = dot_rows(attn_in, grad_qkv)
    qkv_sums = jnp.sum(grad_qkv.astype(F32), axis=0)
    grad_attn_in = dot_back(grad_qkv, weight_qkv)
    grad_ln1_gain = jnp.sum(grad_attn_in * normed1, axis=0)
    grad_ln1_bias = jnp.sum(grad_attn_in, axis=0)
    grad_start = grad_middle + norm_back(grad_attn_in, normed1, rstd1[:, :1], vec[1])
    grad_mask_embed = jnp.sum(grad_start * masked, axis=0)
    patch_grad = (grad_start * (1.0 - masked)).astype(BF)
    return patch_grad, (
        grad_mask_embed,
        grad_ln1_gain,
        grad_ln1_bias,
        grad_w_qkv,
        qkv_sums[:768],
        qkv_sums[1536:],
        grad_w_out,
        grad_bias_out,
        grad_ln2_gain,
        grad_ln2_bias,
        grad_w_fc1,
        grad_bias_fc1,
        grad_w_fc2,
        grad_bias_fc2,
    )


def mask_rows(mask_index, mask_count, seq_len):
    slot_ids = lax.broadcasted_iota(jnp.int32, (1, mask_index.shape[1]), 1)
    valid_slots = (slot_ids < mask_count[:, None]).astype(F32)
    patch_ids = lax.broadcasted_iota(jnp.int32, (1, 1, seq_len), 2)
    onehot = (mask_index[:, :, None] == patch_ids).astype(F32)
    return jnp.einsum("cj,cjp->cp", valid_slots, onehot).reshape(-1, 1)


def kernel_layer(patches, cotangent, mask_index, mask_count, *shards):
    masked = mask_rows(mask_index, mask_count, 512)
    rows = jnp.pad(jnp.stack([shards[i] for i in SMALL]), ((0, 0), (0, 32)))
    small = jnp.pad(jnp.concatenate([rows, shards[11].reshape(3, 128)]), ((0, 4), (0, 0)))
    results = forward_call(patches.reshape(1024, 768), masked, *[shards[i] for i in BIG], small)
    full, kept = results[:4], results[4:]
    patch_grad, grads = backward(cotangent, masked, full, kept)
    shape = patches.shape
    return (kept[10].reshape(shape), patch_grad.reshape(shape)) + kernel_reduce(grads)


def plain_layer(patches, cotangent, mask_index, mask_count, *shards):
    output, patch_grad, grads = compute(patches, cotangent, mask_index, mask_count, plain_gather(shards))
    return (output, patch_grad) + plain_reduce(grads)


def solution(mesh):
    in_specs = (
        P(("narrow", "wide"), None, None),
        P(("narrow", "wide"), None, None),
        P(("narrow", "wide"), None),
        P(("narrow", "wide")),
        P("wide"),
        P("wide"),
        P("wide"),
        P("wide", None),
        P("wide"),
        P("wide"),
        P("wide", None),
        P("wide"),
        P("wide"),
        P("wide"),
        P("wide", None),
        P("wide"),
        P("wide", None),
        P("wide"),
    )
    out_specs = (
        P(("narrow", "wide"), None, None),
        P(("narrow", "wide"), None, None),
        P("wide"),
        P("wide"),
        P("wide"),
        P("wide", None),
        P("wide"),
        P("wide"),
        P("wide", None),
        P("wide"),
        P("wide"),
        P("wide"),
        P("wide", None),
        P("wide"),
        P("wide", None),
        P("wide"),
    )
    kernels = mesh.shape["narrow"] == 4 and mesh.shape["wide"] == 8
    return jax.shard_map(
        kernel_layer if kernels else plain_layer, mesh=mesh, in_specs=in_specs, out_specs=out_specs, check_vma=False
    )
```

```python
import jax
import jax.numpy as jnp
from jax import lax
from jax.experimental import pallas as pl
from jax.experimental.pallas import tpu as pltpu
from jax.sharding import PartitionSpec as P

HEADS = 12
HD = 64


epsilon = 1e-06
inv_root_two = 0.7071067811865476
inv_root_tau = 0.3989422804014327


def dot_rows(left_side, right_side):
    return lax.dot_general(
        left_side, right_side, (((0,), (0,)), ((), ())), preferred_element_type=jnp.float32
    )


def dot_back(left_side, right_side):
    return lax.dot_general(
        left_side, right_side, (((1,), (1,)), ((), ())), preferred_element_type=jnp.float32
    )


def norm_rows(values):
    row_mean = jnp.mean(values, axis=-1, keepdims=True)
    centered = values - row_mean
    variance = jnp.mean(centered * centered, axis=-1, keepdims=True)
    inv_std = lax.rsqrt(variance + epsilon)
    return (centered * inv_std, inv_std)


def norm_back(grad_in, normed, inv_std, ln_gain):
    grad_normed = grad_in * ln_gain[None, :]
    mean_grad = jnp.mean(grad_normed, axis=-1, keepdims=True)
    mean_cross = jnp.mean(grad_normed * normed, axis=-1, keepdims=True)
    return inv_std * (grad_normed - mean_grad - normed * mean_cross)


def split_heads(qkv_clip):
    seq_len = qkv_clip.shape[0]
    split_qkv = qkv_clip.reshape(seq_len, 3, HEADS, HD)
    return (split_qkv[:, 0], split_qkv[:, 1], split_qkv[:, 2])


def clip_scores(query_rows, key_rows):
    return jnp.einsum(
        "qhd,khd->hqk", query_rows, key_rows, preferred_element_type=jnp.float32
    ) * HD ** (-0.5)


def attend(qkv_clip):
    query_rows, key_rows, value_rows = split_heads(qkv_clip)
    scores = clip_scores(query_rows, key_rows)
    row_max = jnp.max(scores, axis=-1, keepdims=True)
    exp_scores = jnp.exp(scores - row_max)
    row_total = jnp.sum(exp_scores, axis=-1, keepdims=True)
    soft_probs = (exp_scores / row_total).astype(jnp.bfloat16)
    attn_mixed = jnp.einsum(
        "hqk,khd->qhd", soft_probs, value_rows, preferred_element_type=jnp.float32
    )
    log_total = (row_max + jnp.log(row_total))[..., 0]
    return (attn_mixed.reshape(qkv_clip.shape[0], HEADS * HD).astype(jnp.bfloat16), log_total)


def attend_back(block_args):
    qkv_clip, grad_mixed, log_total = block_args
    query_rows, key_rows, value_rows = split_heads(qkv_clip)
    grad_heads = grad_mixed.reshape(qkv_clip.shape[0], HEADS, HD)
    soft_probs = jnp.exp(clip_scores(query_rows, key_rows) - log_total[..., None])
    grad_probs = jnp.einsum(
        "qhd,khd->hqk", grad_heads, value_rows, preferred_element_type=jnp.float32
    )
    grad_value = jnp.einsum(
        "hqk,qhd->khd",
        soft_probs.astype(jnp.bfloat16),
        grad_heads,
        preferred_element_type=jnp.float32,
    )
    grad_scores = soft_probs * (
        grad_probs - jnp.sum(soft_probs * grad_probs, axis=-1, keepdims=True)
    )
    grad_scores = grad_scores.astype(jnp.bfloat16)
    grad_query = jnp.einsum(
        "hqk,khd->qhd", grad_scores, key_rows, preferred_element_type=jnp.float32
    ) * HD ** (-0.5)
    grad_key = jnp.einsum(
        "hqk,qhd->khd", grad_scores, query_rows, preferred_element_type=jnp.float32
    ) * HD ** (-0.5)
    stacked = jnp.stack([grad_query, grad_key, grad_value], axis=1)
    return stacked.reshape(qkv_clip.shape[0], 3 * HEADS * HD).astype(jnp.bfloat16)


MESH = pl.DeviceIdType.MESH
BF = jnp.bfloat16
F32 = jnp.float32

UNITS = (
    [("qkv", 768 * j, 0) for j in range(3)]
    + [("out", 0, 0)]
    + [("fc1", 768 * j, 0) for j in range(4)]
    + [("fc2", 0, 96 * j) for j in range(4)]
)
NU = len(UNITS)


def lanes(start):
    return pl.multiple_of(start, 128)


class Place:
    def __init__(self):
        n = lax.axis_index("narrow")
        w = lax.axis_index("wide")
        self.n, self.w = n, w
        self.core, self.x = n % 2, n // 2
        self.y, self.z = w % 2, w // 2
        self.core_peer = (self.x * 2 + (1 - self.core), w)
        self.x_peer = ((1 - self.x) * 2 + self.core, w)
        self.y_peer = (n, self.z * 2 + (1 - self.y))

    def z_up(self, k):
        return (self.z + k) % 4

    def z_peer(self, k):
        return (self.n, self.z_up(k) * 2 + self.y)

    def greet(self):
        barrier = pltpu.get_barrier_semaphore()
        peers = [self.core_peer, self.x_peer, self.y_peer] + [self.z_peer(k) for k in (1, 2, 3)]
        for peer in peers:
            pl.semaphore_signal(barrier, inc=1, device_id=peer, device_id_type=MESH)
        pl.semaphore_wait(barrier, len(peers))


def remote(src, dst, send, recv, peer):
    return pltpu.make_async_remote_copy(
        src_ref=src, dst_ref=dst, send_sem=send, recv_sem=recv, device_id=peer, device_id_type=MESH
    )


class Gather:
    SEMS = [
        pltpu.SemaphoreType.DMA((NU, 10)),
        pltpu.SemaphoreType.DMA((NU, 10)),
        pltpu.SemaphoreType.DMA((NU,)),
        pltpu.SemaphoreType.DMA((8,)),
        pltpu.SemaphoreType.DMA((8,)),
    ]

    def __init__(self, place, shards, full, small, small_full, send, recv, local, ssend, srecv):
        self.p, self.shards, self.full = place, shards, full
        self.small, self.small_full = small, small_full
        self.send, self.recv, self.local, self.ssend, self.srecv = send, recv, local, ssend, srecv
        self.sent = []

    def go(self, u, i, src, dst, peer):
        copy = remote(src, dst, self.send.at[u, i], self.recv.at[u, i], peer)
        copy.start()
        self.sent.append(copy)

    def arrived(self, u, i, dst):
        remote(dst, dst, self.send.at[u, i], self.recv.at[u, i], self.p.x_peer).wait_recv()

    def small_stage(self, stage):
        p = self.p
        if stage == 0:
            own = self.small_full.at[p.z, p.y]
            pltpu.make_async_copy(self.small, own, self.local.at[0]).start()
            pltpu.make_async_copy(self.small, own, self.local.at[0]).wait()
            for k in (1, 2, 3):
                copy = remote(self.small, own, self.ssend.at[k], self.srecv.at[k], p.z_peer(k))
                copy.start()
                self.sent.append(copy)
        elif stage == 1:
            for k in (1, 2, 3):
                dst = self.small_full.at[p.z_up(4 - k), p.y]
                remote(dst, dst, self.ssend.at[k], self.srecv.at[k], p.x_peer).wait_recv()
            mine = self.small_full.at[:, p.y]
            copy = remote(mine, mine, self.ssend.at[0], self.srecv.at[0], p.y_peer)
            copy.start()
            self.sent.append(copy)
        else:
            dst = self.small_full.at[:, 1 - p.y]
            remote(dst, dst, self.ssend.at[0], self.srecv.at[0], p.x_peer).wait_recv()

    def stage(self, u, stage):
        p = self.p
        name, co, ro = UNITS[u]
        full, shard = self.full[name], self.shards[name]
        rows = pl.ds(ro, 96)
        own = pl.ds(lanes(co + p.core * 384 + p.x * 128), 256)
        exc = pl.ds(lanes(co + p.core * 384 + p.x * 256), 128)
        peer_exc = pl.ds(lanes(co + p.core * 384 + (1 - p.x) * 256), 128)
        oth = pl.ds(lanes(co + (1 - p.core) * 384 + p.x * 128), 256)
        oth_exc = pl.ds(lanes(co + (1 - p.core) * 384 + (1 - p.x) * 256), 128)
        if stage == 0:
            mine = shard.at[rows, own]
            home = full.at[p.z, p.y, rows, own]
            pltpu.make_async_copy(mine, home, self.local.at[u]).start()
            for k in (1, 2, 3):
                self.go(u, k, mine, home, p.z_peer(k))
        elif stage == 1:
            home = full.at[p.z, p.y, rows, own]
            pltpu.make_async_copy(shard.at[rows, own], home, self.local.at[u]).wait()
            for k in (1, 2, 3):
                self.arrived(u, k, full.at[p.z_up(4 - k), p.y, rows, own])
            column = full.at[:, p.y, rows, own]
            part = full.at[:, p.y, rows, exc]
            self.go(u, 0, column, column, p.y_peer)
            self.go(u, 4, part, part, p.x_peer)
            self.go(u, 5, column, column, p.core_peer)
        elif stage == 2:
            column = full.at[:, 1 - p.y, rows, own]
            part = full.at[:, 1 - p.y, rows, exc]
            self.arrived(u, 0, column)
            self.go(u, 6, part, part, p.x_peer)
            self.go(u, 7, column, column, p.core_peer)
        elif stage == 3:
            self.arrived(u, 4, full.at[:, p.y, rows, peer_exc])
            self.arrived(u, 6, full.at[:, 1 - p.y, rows, peer_exc])
            both = full.at[:, :, rows, peer_exc]
            self.go(u, 8, both, both, p.core_peer)
        else:
            self.arrived(u, 5, full.at[:, p.y, rows, oth])
            self.arrived(u, 7, full.at[:, 1 - p.y, rows, oth])
            self.arrived(u, 8, full.at[:, :, rows, oth_exc])

    def finish(self):
        for copy in self.sent:
            copy.wait_send()


class Reduce:
    SCRATCH = [
        pltpu.VMEM((NU, 4, 2, 96, 384), BF),
        pltpu.VMEM((NU, 4, 2, 96, 128), BF),
        pltpu.VMEM((NU, 4, 96, 256), BF),
        pltpu.VMEM((NU, 3, 96, 256), BF),
        pltpu.VMEM((NU, 2, 96, 256), BF),
        pltpu.VMEM((NU, 2, 96, 384), BF),
        pltpu.VMEM((10, 16, 768), F32),
        pltpu.SemaphoreType.DMA((NU, 8)),
        pltpu.SemaphoreType.DMA((NU, 8)),
        pltpu.SemaphoreType.DMA((6,)),
        pltpu.SemaphoreType.DMA((6,)),
    ]

    def __init__(self, place, grads, outs, staging, out_sem, bufs):
        self.p, self.grads, self.outs = place, grads, outs
        self.staging, self.out_sem, self.leaving = staging, out_sem, []
        (self.c, self.xb, self.yb, self.zb, self.f, self.e, self.s,
         self.send, self.recv, self.ssend, self.srecv) = bufs
        self.sent = []

    def go(self, u, i, src, dst, peer):
        copy = remote(src, dst, self.send.at[u, i], self.recv.at[u, i], peer)
        copy.start()
        self.sent.append(copy)

    def arrived(self, u, i, dst):
        remote(dst, dst, self.send.at[u, i], self.recv.at[u, i], self.p.x_peer).wait_recv()

    def stage(self, u, stage):
        p = self.p
        name, co, ro = RUNITS[u]
        grad = self.grads[name]
        rows = pl.ds(ro, 96)
        own = pl.ds(lanes(co + p.core * 384), 384)
        oth = pl.ds(lanes(co + (1 - p.core) * 384), 384)
        exc = pl.ds(lanes(p.x * 256), 128)
        peer_exc = pl.ds(lanes((1 - p.x) * 256), 128)
        two = pl.ds(lanes(p.x * 128), 256)
        c, xb, yb, zb = self.c.at[u], self.xb.at[u], self.yb.at[u], self.zb.at[u]
        if stage == 0:
            self.go(u, 0, grad.at[:, :, rows, oth], c, p.core_peer)
        elif stage == 1:
            self.arrived(u, 0, c)

            def add(i, carry):
                a, b = i // 2, i % 2
                c[a, b] = (c[a, b].astype(F32) + grad[a, b, rows, own].astype(F32)).astype(BF)
                return carry

            lax.fori_loop(0, 8, add, 0)
            self.go(u, 1, c.at[:, :, :, peer_exc], xb, p.x_peer)
        elif stage == 2:
            self.arrived(u, 1, xb)

            def add(i, carry):
                a, b = i // 2, i % 2
                c[a, b, :, exc] = (c[a, b, :, exc].astype(F32) + xb[a, b].astype(F32)).astype(BF)
                return carry

            lax.fori_loop(0, 8, add, 0)
            self.go(u, 2, c.at[:, 1 - p.y, :, two], yb, p.y_peer)
        elif stage == 3:
            self.arrived(u, 2, yb)

            def add(a, carry):
                c[a, p.y, :, two] = (c[a, p.y, :, two].astype(F32) + yb[a].astype(F32)).astype(BF)
                return carry

            lax.fori_loop(0, 4, add, 0)
            for k in (1, 2, 3):
                self.go(u, 2 + k, c.at[p.z_up(k), p.y, :, two], zb.at[k - 1], p.z_peer(k))
        elif stage == 4:
            for k in (1, 2, 3):
                self.arrived(u, 2 + k, zb.at[k - 1])
            total = c[p.z, p.y, :, two].astype(F32)
            for k in (1, 2, 3):
                total = total + zb[k - 1].astype(F32)
            self.f[u, 0] = total.astype(BF)
            self.go(u, 6, self.f.at[u, 0], self.f.at[u, 1], p.x_peer)
        elif stage == 5:
            self.arrived(u, 6, self.f.at[u, 1])
            low = self.f[u, p.x].astype(F32)
            high = self.f[u, 1 - p.x].astype(F32)
            self.e[u, 0, :, 0:128] = low[:, 0:128].astype(BF)
            self.e[u, 0, :, 128:256] = (low[:, 128:] + high[:, :128]).astype(BF)
            self.e[u, 0, :, 256:384] = high[:, 128:].astype(BF)
            self.go(u, 7, self.e.at[u, 0], self.e.at[u, 1], p.core_peer)
        else:
            self.arrived(u, 7, self.e.at[u, 1])
            slot = self.staging.at[u % 3]
            if u >= 3:
                self.leaving[u - 3].wait()
            slot[:, pl.ds(lanes(p.core * 384), 384)] = self.e[u, 0].astype(F32)
            slot[:, pl.ds(lanes((1 - p.core) * 384), 384)] = self.e[u, 1].astype(F32)
            target = self.outs[name].at[rows, pl.ds(co, 768)]
            copy = pltpu.make_async_copy(slot, target, self.out_sem.at[u])
            copy.start()
            self.leaving.append(copy)

    def small_stage(self, stage, mine=None):
        p, s = self.p, self.s
        peers = [p.core_peer, p.x_peer, p.y_peer]
        if stage == 0:
            s[0] = mine
        elif stage <= 3:
            i = stage - 1
            dst = s.at[2 * i + 1]
            remote(dst, dst, self.ssend.at[i], self.srecv.at[i], p.x_peer).wait_recv()
            s[2 * i + 2] = s[2 * i] + s[2 * i + 1]
        if stage < 3:
            copy = remote(s.at[2 * stage], s.at[2 * stage + 1], self.ssend.at[stage], self.srecv.at[stage], peers[stage])
            copy.start()
            self.sent.append(copy)
        elif stage == 3:
            for k in (1, 2, 3):
                copy = remote(s.at[6], s.at[6 + k], self.ssend.at[2 + k], self.srecv.at[2 + k], p.z_peer(k))
                copy.start()
                self.sent.append(copy)
        else:
            total = s[6]
            for k in (1, 2, 3):
                dst = s.at[6 + k]
                remote(dst, dst, self.ssend.at[2 + k], self.srecv.at[2 + k], p.x_peer).wait_recv()
                total = total + s[6 + k]
            return total

    def finish(self):
        for copy in self.sent:
            copy.wait_send()
        for copy in self.leaving[-3:]:
            copy.wait()


def kernel_params(cid, side=True):
    return pltpu.CompilerParams(collective_id=cid, has_side_effects=side, vmem_limit_bytes=67043328)


VM = pl.BlockSpec(memory_space=pltpu.VMEM)
ANY = pl.BlockSpec(memory_space=pl.ANY)
NAMES = ("qkv", "out", "fc1", "fc2")
FULL = {"qkv": (4, 2, 96, 2304), "out": (4, 2, 96, 768), "fc1": (4, 2, 96, 3072), "fc2": (4, 2, 384, 768)}


def row_block(i, size):
    return pl.ds(pl.multiple_of(i * size, size), size)


class Ticks:
    def __init__(self, run, stages, ahead):
        self.run, self.stages, self.ahead = run, stages, ahead
        self.t = 0
        for u in range(ahead):
            run(u, 0)

    def tick(self):
        t = self.t
        self.t += 1
        if t + self.ahead < NU:
            self.run(t + self.ahead, 0)
        for s in range(1, self.stages):
            if 0 <= t - s + 1 < NU:
                self.run(t - s + 1, s)

    def need(self, u):
        while self.t < u + self.stages - 1:
            self.tick()


def matmul(left, right):
    return jnp.dot(left, right, preferred_element_type=F32)


def norm_block(values):
    mean = jnp.mean(values, axis=1, keepdims=True)
    centered = values - mean
    variance = jnp.mean(centered * centered, axis=1, keepdims=True)
    inv_std = lax.rsqrt(variance + epsilon)
    return centered * inv_std, inv_std


KEPT = (
    ("attn_in", (1024, 768), BF),
    ("normed1", (1024, 768), BF),
    ("rstd1", (1024, 128), F32),
    ("qkv", (1024, 2304), BF),
    ("mixed", (1024, 768), BF),
    ("mlp_in", (1024, 768), BF),
    ("normed2", (1024, 768), BF),
    ("rstd2", (1024, 128), F32),
    ("act", (1024, 3072), BF),
    ("slope", (1024, 3072), BF),
    ("out", (1024, 768), BF),
    ("vec", (16, 768), F32),
)


def attend_pair(qkv, mixed, i):
    clip, pair = i // 6, i % 6
    rows = row_block(clip, 512)
    at = pl.multiple_of(pair * 128, 128)
    q2 = qkv[rows, pl.ds(at, 128)]
    k2 = qkv[rows, pl.ds(pl.multiple_of(at + 768, 128), 128)]
    v2 = qkv[rows, pl.ds(pl.multiple_of(at + 1536, 128), 128)]
    lane = lax.broadcasted_iota(jnp.int32, (512, 128), 1)
    parts = []
    for h in range(2):
        inside = (lane >= 64) if h else (lane < 64)
        qh = jnp.where(inside, q2 * jnp.asarray(0.125, BF), jnp.zeros_like(q2))
        scores = lax.dot_general(qh, k2, (((1,), (1,)), ((), ())), preferred_element_type=F32)
        e = jnp.exp(scores - jnp.max(scores, axis=1, keepdims=True))
        total = jnp.sum(e, axis=1, keepdims=True)
        parts.append(matmul(e.astype(BF), v2) * (1.0 / total))
    mixed[rows, pl.ds(at, 128)] = jnp.where(lane < 64, parts[0], parts[1]).astype(BF)


def forward_kernel(*refs):
    patches, mask = refs[0:2]
    shards = dict(zip(NAMES, refs[2:6]))
    small = refs[6]
    n_out = 4 + len(KEPT)
    full_out = dict(zip(NAMES, refs[7:11]))
    kept_out = dict(zip([k[0] for k in KEPT], refs[11 : 7 + n_out]))
    rest = refs[7 + n_out :]
    full = dict(zip(NAMES, rest[0:4]))
    kept = dict(zip([k[0] for k in KEPT], rest[4 : 4 + len(KEPT)]))
    middle, small_full, bias1, out_sem = rest[4 + len(KEPT) : 8 + len(KEPT)]
    sems = rest[8 + len(KEPT) :]
    place = Place()
    place.greet()
    g = Gather(place, shards, full, small, small_full, *sems)
    leaving = []

    def leave(src, dst):
        copy = pltpu.make_async_copy(src, dst, out_sem.at[len(leaving)])
        copy.start()
        leaving.append(copy)

    def keep(name):
        leave(kept[name], kept_out[name])

    g.small_stage(0)
    ticks = Ticks(g.stage, 5, 3)
    g.small_stage(1)
    g.small_stage(2)
    ticks.tick()
    vec = kept["vec"]
    total = jnp.zeros((16, 768), F32)
    spot = lax.broadcasted_iota(jnp.int32, (128, 768), 1) - lax.broadcasted_iota(jnp.int32, (128, 768), 0)
    inside = lax.broadcasted_iota(jnp.int32, (128, 768), 0) < 96
    for s in range(8):
        block = small_full[s // 2, s % 2]
        pick = jnp.where((spot == 96 * s) & inside, 1.0, 0.0).astype(BF)
        total = total + matmul(block, pick)
        wide = block.astype(F32)
        for r in range(3):
            bias1[:, pl.ds(s * 384 + r * 128, 128)] = jnp.broadcast_to(wide[9 + r : 10 + r, :], (8, 128))
    vec[...] = total
    keep("vec")

    def norm1(i, carry):
        rows = row_block(i, 128)
        m = mask[rows, 0:1]
        start = patches[rows, :].astype(F32) * (1.0 - m) + m * vec[0:1, :]
        normed, inv_std = norm_block(start)
        middle[rows, :] = start
        kept["normed1"][rows, :] = normed.astype(BF)
        kept["rstd1"][rows, :] = jnp.broadcast_to(inv_std, (128, 128))
        kept["attn_in"][rows, :] = (normed * vec[1:2, :] + vec[2:3, :]).astype(BF)
        return carry

    lax.fori_loop(0, 8, norm1, 0)
    for name in ("attn_in", "normed1", "rstd1"):
        keep(name)
    for u in range(3):
        ticks.need(u)
        w = full["qkv"][:, :, :, pl.ds(768 * u, 768)].reshape(768, 768)

        def project(i, carry):
            rows = row_block(i, 512)
            value = matmul(kept["attn_in"][rows, :], w)
            if u != 1:
                row = 3 if u == 0 else 4
                value = value + vec[row : row + 1, :]
            kept["qkv"][rows, pl.ds(768 * u, 768)] = value.astype(BF)
            return carry

        lax.fori_loop(0, 2, project, 0)
    leave(full["qkv"], full_out["qkv"])
    keep("qkv")
    for part in range(6):

        def attend_two(i, carry):
            attend_pair(kept["qkv"], kept["mixed"], i)
            return carry

        lax.fori_loop(2 * part, 2 * part + 2, attend_two, 0)
        ticks.tick()
    keep("mixed")
    ticks.need(3)
    leave(full["out"], full_out["out"])
    w_out = full["out"][...].reshape(768, 768)

    def mix(i, carry):
        rows = row_block(i, 512)
        middle[rows, :] = middle[rows, :] + (matmul(kept["mixed"][rows, :], w_out) + vec[5:6, :])
        return carry

    lax.fori_loop(0, 2, mix, 0)
    ticks.tick()

    def norm2(i, carry):
        rows = row_block(i, 128)
        normed, inv_std = norm_block(middle[rows, :])
        kept["normed2"][rows, :] = normed.astype(BF)
        kept["rstd2"][rows, :] = jnp.broadcast_to(inv_std, (128, 128))
        kept["mlp_in"][rows, :] = (normed * vec[6:7, :] + vec[7:8, :]).astype(BF)
        return carry

    lax.fori_loop(0, 8, norm2, 0)
    for name in ("normed2", "rstd2", "mlp_in"):
        keep(name)
    for j in range(4):
        ticks.need(4 + j)
        w = full["fc1"][:, :, :, pl.ds(768 * j, 768)].reshape(768, 768)

        def expand(i, carry):
            rows = row_block(i, 256)
            cols = pl.ds(768 * j, 768)
            h = matmul(kept["mlp_in"][rows, :], w) + bias1[0:1, cols]
            below = 0.5 * (1.0 + lax.erf(h * inv_root_two))
            density = jnp.exp(-0.5 * h * h) * inv_root_tau
            kept["act"][rows, cols] = (h * below).astype(BF)
            kept["slope"][rows, cols] = (below + h * density).astype(BF)
            return carry

        lax.fori_loop(0, 4, expand, 0)
        ticks.tick()
    leave(full["fc1"], full_out["fc1"])
    keep("act")
    keep("slope")
    ticks.need(NU - 1)
    leave(full["fc2"], full_out["fc2"])

    def contract(i, carry):
        rows = row_block(i, 512)
        value = middle[rows, :] + vec[8:9, :]
        for k in range(4):
            w = full["fc2"][k].reshape(768, 768)
            value = value + matmul(kept["act"][rows, pl.ds(768 * k, 768)], w)
        kept["out"][rows, :] = value.astype(BF)
        return carry

    lax.fori_loop(0, 2, contract, 0)
    keep("out")
    g.finish()
    for copy in leaving:
        copy.wait()


def forward_call(patches, mask, qkv, out, fc1, fc2, small):
    shapes = [jax.ShapeDtypeStruct(FULL[k], BF) for k in NAMES]
    shapes += [jax.ShapeDtypeStruct(k[1], k[2]) for k in KEPT]
    scratch = [pltpu.VMEM(FULL[k], BF) for k in NAMES]
    scratch += [pltpu.VMEM(k[1], k[2]) for k in KEPT]
    scratch += [
        pltpu.VMEM((1024, 768), F32),
        pltpu.VMEM((4, 2, 16, 128), BF),
        pltpu.VMEM((8, 3072), F32),
        pltpu.SemaphoreType.DMA((4 + len(KEPT),)),
    ]
    return pl.pallas_call(
        forward_kernel,
        out_shape=shapes,
        in_specs=[VM] * 7,
        out_specs=[ANY] * len(shapes),
        scratch_shapes=scratch + Gather.SEMS,
        compiler_params=kernel_params(0),
        name="forward",
    )(patches, mask, qkv, out, fc1, fc2, small)

RUNITS = UNITS[8:12] + UNITS[4:8] + UNITS[3:4] + UNITS[0:3]


class Service:
    def __init__(self, run, stages):
        self.run, self.stages = run, stages
        self.ready, self.at = 0, []

    def call(self):
        if len(self.at) < self.ready:
            self.at.append(0)
        for u in reversed(range(len(self.at))):
            if self.at[u] < self.stages:
                self.run(u, self.at[u])
                self.at[u] += 1

    def busy(self):
        return len(self.at) < self.ready or any(a < self.stages for a in self.at)


def attend_pair_back(qkv, mixed, grad_mixed, grad_qkv, sums, acc, i):
    clip, pair = i // 6, i % 6
    rows = row_block(clip, 512)
    at = pl.multiple_of(pair * 128, 128)
    spots = [pl.ds(pl.multiple_of(at + 768 * p, 128), 128) for p in range(3)]
    acc[...] = jnp.zeros_like(acc)

    def part(n, carry):
        head, block = n // 2, n % 2
        q_rows = pl.ds(pl.multiple_of(clip * 512 + block * 256, 256), 256)
        inside = lax.broadcasted_iota(jnp.int32, (256, 128), 1) // 64 == head
        inside_keys = lax.broadcasted_iota(jnp.int32, (512, 128), 1) // 64 == head
        q2 = qkv[q_rows, spots[0]]
        k2 = qkv[rows, spots[1]]
        v2 = qkv[rows, spots[2]]
        grad2 = grad_mixed[q_rows, pl.ds(at, 128)]
        out2 = mixed[q_rows, pl.ds(at, 128)]
        eighth = jnp.asarray(0.125, BF)
        qh = jnp.where(inside, q2 * eighth, jnp.zeros_like(q2))
        gh = jnp.where(inside, grad2, jnp.zeros_like(grad2))
        kh = jnp.where(inside_keys, k2 * eighth, jnp.zeros_like(k2))
        scores = dot_back(k2, qh)
        e = jnp.exp(scores - jnp.max(scores, axis=0, keepdims=True))
        probs = e * (1.0 / jnp.sum(e, axis=0, keepdims=True))
        shared = lax.dot_general(
            jnp.ones((8, 128), F32),
            gh.astype(F32) * out2.astype(F32),
            (((1,), (1,)), ((), ())),
            precision=lax.Precision.HIGHEST,
            preferred_element_type=F32,
        )[0:1, :]
        grad_scores = (probs * (dot_back(v2, gh) - shared)).astype(BF)
        acc[2] += matmul(probs.astype(BF), gh)
        acc[1] += matmul(grad_scores, qh)
        acc[0, pl.ds(pl.multiple_of(block * 256, 256), 256), :] += dot_rows(grad_scores, kh)
        return carry

    lax.fori_loop(0, 4, part, 0)
    for p in range(3):
        value = acc[p].astype(BF)
        grad_qkv[rows, spots[p]] = value
        if p != 1:
            row = 3 if p == 0 else 4
            sums[row : row + 1, pl.ds(at, 128)] += jnp.sum(value.astype(F32), axis=0, keepdims=True)


def backward_kernel(*refs):
    vec, mask = refs[0:2]
    names = ("cot", "attn_in", "normed1", "rstd1", "qkv", "mixed", "mlp_in", "normed2", "rstd2", "act", "slope")
    held = dict(zip(names, refs[2:13]))
    weights = dict(zip(NAMES, refs[13:17]))
    outs = dict(zip(NAMES, refs[17:21]))
    small_out, patch_out = refs[21:23]
    (cot, act, slope, w2, w1, mlp_in, normed2, rstd2, mixed, total, sums, acc,
     g_fc2, g_fc1, g_out, staging, load_sem, out_sem) = refs[23:41]
    place = Place()
    place.greet()
    grads = {"qkv": w1, "out": g_out, "fc1": g_fc1, "fc2": g_fc2}
    r = Reduce(place, grads, outs, staging, out_sem, refs[41:])
    svc = Service(r.stage, 7)
    loads = {}

    def load(name, src, dst):
        copy = pltpu.make_async_copy(src, dst, load_sem.at[len(loads)])
        copy.start()
        loads[name] = copy

    def loaded(*names):
        for name in names:
            loads[name].wait()

    load("cot", held["cot"], cot)
    load("act", held["act"], act)
    load("fc2", weights["fc2"], w2)
    load("slope", held["slope"], slope)
    load("mlp_in", held["mlp_in"], mlp_in)
    load("fc1", weights["fc1"], w1)
    load("normed2", held["normed2"], normed2)
    load("rstd2", held["rstd2"], rstd2)
    load("mixed", held["mixed"], mixed)
    sums[...] = jnp.zeros_like(sums)
    loaded("cot", "act")

    def weight_fc2(i, carry):
        left = act[:, pl.ds(pl.multiple_of(i * 384, 128), 384)]
        g_fc2[i // 2, i % 2] = dot_rows(left, cot[...]).astype(BF)
        return carry

    lax.fori_loop(0, 8, weight_fc2, 0)

    def bias_fc2(i, carry):
        sums[8:9, :] += jnp.sum(cot[row_block(i, 256), :].astype(F32), axis=0, keepdims=True)
        return carry

    lax.fori_loop(0, 4, bias_fc2, 0)
    svc.ready = 4
    svc.call()
    loaded("fc2", "slope", "mlp_in", "fc1")

    def weight_grad(left, right, target):
        def some(i, carry):
            rows = left[:, pl.ds(pl.multiple_of(i * 384, 128), 384)]
            value = dot_rows(rows, right()).astype(BF).reshape(2, 2, 96, 768)
            target(pl.ds(2 * i, 2), value)
            return carry

        lax.fori_loop(0, 2, some, 0)

    for j in range(4):
        cols = pl.ds(768 * j, 768)

        def hidden(i, carry):
            rows = row_block(i, 512)
            value = dot_back(cot[rows, :], w2[j].reshape(768, 768)) * slope[rows, cols].astype(F32)
            value = value.astype(BF)
            slope[rows, cols] = value
            sums[9 + j : 10 + j, :] += jnp.sum(value.astype(F32), axis=0, keepdims=True)
            return carry

        lax.fori_loop(0, 2, hidden, 0)
        if j == 3:
            for p in range(3):
                load(f"w{p}", weights["qkv"].at[:, :, :, pl.ds(768 * p, 768)], w2.at[:, :, pl.ds(96 * p, 96), :])
            load("w3", weights["out"], w2.at[:, :, pl.ds(288, 96), :])

        def put_fc1(z, value):
            g_fc1[z, :, :, cols] = value

        weight_grad(mlp_in, lambda: slope[:, cols], put_fc1)
        svc.ready = 5 + j
        svc.call()

        def spread(i, carry):
            rows = row_block(i, 512)
            value = dot_back(slope[rows, cols], w1[:, :, :, cols].reshape(768, 768))
            total[rows, :] = value if j == 0 else total[rows, :] + value
            return carry

        lax.fori_loop(0, 2, spread, 0)
    load("qkv", held["qkv"], slope.at[:, pl.ds(0, 2304)])
    svc.call()
    loaded("normed2", "rstd2")

    def norm_step(grad, normed, inv_std, gain):
        scaled = grad * gain
        mean = jnp.mean(scaled, axis=1, keepdims=True)
        cross = jnp.mean(scaled * normed, axis=1, keepdims=True)
        return inv_std * (scaled - mean - normed * cross)

    def column_sum(row, value):
        sums[row : row + 1, :] += jnp.sum(value, axis=0, keepdims=True)

    def norm2(i, carry):
        rows = row_block(i, 128)
        grad, normed = total[rows, :], normed2[rows, :].astype(F32)
        column_sum(6, grad * normed)
        column_sum(7, grad)
        middle = cot[rows, :].astype(F32) + norm_step(grad, normed, rstd2[rows, 0:1], vec[6:7, :])
        total[rows, :] = middle
        branch = middle.astype(BF)
        mlp_in[rows, :] = branch
        column_sum(5, branch.astype(F32))
        return carry

    lax.fori_loop(0, 8, norm2, 0)
    load("normed1", held["normed1"], normed2)
    load("rstd1", held["rstd1"], rstd2)
    loaded("mixed", "w3")

    def put_out(z, value):
        g_out[z] = value

    weight_grad(mixed, lambda: mlp_in[...], put_out)
    svc.ready = 9

    def branch_back(i, carry):
        rows = row_block(i, 512)
        w = w2[:, :, pl.ds(288, 96), :].reshape(768, 768)
        cot[rows, :] = dot_back(mlp_in[rows, :], w).astype(BF)
        return carry

    lax.fori_loop(0, 2, branch_back, 0)
    svc.call()
    load("attn_in", held["attn_in"], mlp_in)
    loaded("qkv")
    for n in range(6):

        def attend_two(i, carry):
            attend_pair_back(slope, mixed, cot, act, sums, acc, i)
            return carry

        lax.fori_loop(2 * n, 2 * n + 2, attend_two, 0)
        svc.call()
    loaded("attn_in", "w0", "w1", "w2", "normed1", "rstd1")
    for p in range(3):
        cols = pl.ds(768 * p, 768)

        def put_qkv(z, value):
            w1[z, :, :, cols] = value

        weight_grad(mlp_in, lambda: act[:, cols], put_qkv)
        svc.ready = 10 + p
        svc.call()

    def norm1(i, carry):
        rows = row_block(i, 256)
        grad = jnp.zeros((256, 768), F32)
        for p in range(3):
            w = w2[:, :, pl.ds(96 * p, 96), :].reshape(768, 768)
            grad = grad + dot_back(act[rows, pl.ds(768 * p, 768)], w)
        normed = normed2[rows, :].astype(F32)
        column_sum(1, grad * normed)
        column_sum(2, grad)
        start = total[rows, :] + norm_step(grad, normed, rstd2[rows, 0:1], vec[1:2, :])
        m = mask[rows, 0:1]
        column_sum(0, start * m)
        mixed[rows, :] = (start * (1.0 - m)).astype(BF)
        return carry

    lax.fori_loop(0, 2, norm1, 0)
    svc.call()
    lax.fori_loop(2, 4, norm1, 0)
    load("patch", mixed, patch_out)
    small_stage = 0
    while svc.busy() or small_stage < 5:
        if small_stage == 0:
            r.small_stage(0, sums[...])
        elif small_stage < 4:
            r.small_stage(small_stage)
        elif small_stage == 4:
            small_out[...] = r.small_stage(4)
        small_stage += 1
        svc.call()
    loaded("patch")
    r.finish()


def backward_call(vec, mask, held, full):
    scratch = [
        pltpu.VMEM((1024, 768), BF),
        pltpu.VMEM((1024, 3072), BF),
        pltpu.VMEM((1024, 3072), BF),
        pltpu.VMEM(FULL["fc2"], BF),
        pltpu.VMEM(FULL["fc1"], BF),
        pltpu.VMEM((1024, 768), BF),
        pltpu.VMEM((1024, 768), BF),
        pltpu.VMEM((1024, 128), F32),
        pltpu.VMEM((1024, 768), BF),
        pltpu.VMEM((1024, 768), F32),
        pltpu.VMEM((16, 768), F32),
        pltpu.VMEM((3, 512, 128), F32),
        pltpu.VMEM(FULL["fc2"], BF),
        pltpu.VMEM(FULL["fc1"], BF),
        pltpu.VMEM(FULL["out"], BF),
        pltpu.VMEM((3, 96, 768), F32),
        pltpu.SemaphoreType.DMA((20,)),
        pltpu.SemaphoreType.DMA((NU,)),
    ]
    shapes = [jax.ShapeDtypeStruct(SHARD[k], F32) for k in NAMES]
    shapes += [jax.ShapeDtypeStruct((16, 768), F32), jax.ShapeDtypeStruct((1024, 768), BF)]
    return pl.pallas_call(
        backward_kernel,
        out_shape=shapes,
        in_specs=[VM] * 2 + [ANY] * 15,
        out_specs=[ANY] * 4 + [VM, ANY],
        scratch_shapes=scratch + Reduce.SCRATCH,
        compiler_params=kernel_params(1),
        name="backward",
    )(vec, mask, *held, *full)


SHARD = {"qkv": (96, 2304), "out": (96, 768), "fc1": (96, 3072), "fc2": (384, 768)}


def compute(patches, cotangent, mask_index, mask_count, gathered):
    (
        embed_full,
        gain_attn,
        shift_attn,
        weight_qkv,
        query_bias,
        value_bias,
        weight_out,
        out_bias,
        gain_mlp,
        shift_mlp,
        weight_fc1,
        fc1_bias,
        weight_fc2,
        fc2_bias,
    ) = gathered
    clip_count, seq_len, feature_count = patches.shape
    row_count = clip_count * seq_len
    slot_ids = lax.broadcasted_iota(jnp.int32, (1, mask_index.shape[1]), 1)
    valid_slots = (slot_ids < mask_count[:, None]).astype(jnp.float32)
    patch_ids = lax.broadcasted_iota(jnp.int32, (1, 1, seq_len), 2)
    onehot = (mask_index[:, :, None] == patch_ids).astype(jnp.float32)
    masked = jnp.einsum("cj,cjp->cp", valid_slots, onehot).reshape(row_count, 1)
    kept_rows = 1.0 - masked
    start_rows = (
        patches.reshape(row_count, feature_count).astype(jnp.float32) * kept_rows
        + masked * embed_full.astype(jnp.float32)[None, :]
    )
    normed_attn, rstd_attn = norm_rows(start_rows)
    attn_in = (
        normed_attn * gain_attn.astype(jnp.float32)[None, :]
        + shift_attn.astype(jnp.float32)[None, :]
    ).astype(jnp.bfloat16)
    qkv_bias = jnp.concatenate([query_bias, jnp.zeros_like(query_bias), value_bias]).astype(
        jnp.float32
    )
    qkv = (
        jnp.dot(attn_in, weight_qkv, preferred_element_type=jnp.float32) + qkv_bias[None, :]
    ).astype(jnp.bfloat16)
    qkv_clips = qkv.reshape(clip_count, seq_len, 3 * feature_count)
    attn_mixed, log_total = lax.map(attend, qkv_clips)
    attn_mixed = attn_mixed.reshape(row_count, feature_count)
    middle = start_rows + (
        jnp.dot(attn_mixed, weight_out, preferred_element_type=jnp.float32)
        + out_bias.astype(jnp.float32)[None, :]
    )
    normed_mlp, rstd_mlp = norm_rows(middle)
    mlp_in = (
        normed_mlp * gain_mlp.astype(jnp.float32)[None, :] + shift_mlp.astype(jnp.float32)[None, :]
    ).astype(jnp.bfloat16)
    hidden = (
        jnp.dot(mlp_in, weight_fc1, preferred_element_type=jnp.float32)
        + fc1_bias.astype(jnp.float32)[None, :]
    )
    activated = jax.nn.gelu(hidden, approximate=False).astype(jnp.bfloat16)
    result = middle + (
        jnp.dot(activated, weight_fc2, preferred_element_type=jnp.float32)
        + fc2_bias.astype(jnp.float32)[None, :]
    )
    output = result.astype(jnp.bfloat16).reshape(clip_count, seq_len, feature_count)
    grad_result = cotangent.reshape(row_count, feature_count)
    grad_w_fc2 = dot_rows(activated, grad_result)
    grad_bias_fc2 = jnp.sum(grad_result.astype(jnp.float32), axis=0)
    grad_act = dot_back(grad_result, weight_fc2)
    gelu_slope = (
        0.5 * (1.0 + lax.erf(hidden * inv_root_two))
        + hidden * jnp.exp(-0.5 * hidden * hidden) * inv_root_tau
    )
    grad_hidden = (grad_act * gelu_slope).astype(jnp.bfloat16)
    grad_w_fc1 = dot_rows(mlp_in, grad_hidden)
    grad_bias_fc1 = jnp.sum(grad_hidden.astype(jnp.float32), axis=0)
    grad_mlp_in = dot_back(grad_hidden, weight_fc1)
    grad_ln2_gain = jnp.sum(grad_mlp_in * normed_mlp, axis=0)
    grad_ln2_bias = jnp.sum(grad_mlp_in, axis=0)
    grad_middle = grad_result.astype(jnp.float32) + norm_back(
        grad_mlp_in, normed_mlp, rstd_mlp, gain_mlp.astype(jnp.float32)
    )
    grad_branch = grad_middle.astype(jnp.bfloat16)
    grad_w_out = dot_rows(attn_mixed, grad_branch)
    grad_bias_out = jnp.sum(grad_branch.astype(jnp.float32), axis=0)
    grad_mixed = dot_back(grad_branch, weight_out).astype(jnp.bfloat16)
    grad_qkv = lax.map(
        attend_back, (qkv_clips, grad_mixed.reshape(clip_count, seq_len, feature_count), log_total)
    )
    grad_qkv = grad_qkv.reshape(row_count, 3 * feature_count)
    grad_w_qkv = dot_rows(attn_in, grad_qkv)
    qkv_sums = jnp.sum(grad_qkv.astype(jnp.float32), axis=0)
    grad_bias_q = qkv_sums[:feature_count]
    grad_bias_v = qkv_sums[2 * feature_count :]
    grad_attn_in = dot_back(grad_qkv, weight_qkv)
    grad_ln1_gain = jnp.sum(grad_attn_in * normed_attn, axis=0)
    grad_ln1_bias = jnp.sum(grad_attn_in, axis=0)
    grad_start = grad_middle + norm_back(
        grad_attn_in, normed_attn, rstd_attn, gain_attn.astype(jnp.float32)
    )
    grad_mask_embed = jnp.sum(grad_start * masked, axis=0)
    patch_grad = (
        (grad_start * kept_rows).astype(jnp.bfloat16).reshape(clip_count, seq_len, feature_count)
    )
    return output, patch_grad, (
        grad_mask_embed,
        grad_ln1_gain,
        grad_ln1_bias,
        grad_w_qkv,
        grad_bias_q,
        grad_bias_v,
        grad_w_out,
        grad_bias_out,
        grad_ln2_gain,
        grad_ln2_bias,
        grad_w_fc1,
        grad_bias_fc1,
        grad_w_fc2,
        grad_bias_fc2,
    )


def plain_gather(shards):
    return tuple(lax.all_gather(s, "wide", axis=0, tiled=True) for s in shards)


def plain_reduce(grads):
    shards = [lax.psum_scatter(g, "wide", scatter_dimension=0, tiled=True) for g in grads]
    return tuple(lax.psum(s.astype(BF), "narrow").astype(F32) for s in shards)


SMALL = (0, 1, 2, 4, 5, 7, 8, 9, 13)
BIG = (3, 6, 10, 12)


def place_small(total):
    place = lax.axis_index("wide")
    mine = lax.dynamic_slice(total, (0, place * 96), (9, 96))
    return mine, lax.dynamic_slice(total[9:13].reshape(3072), (place * 384,), (384,))


def mask_rows(mask_index, mask_count, seq_len):
    slot_ids = lax.broadcasted_iota(jnp.int32, (1, mask_index.shape[1]), 1)
    valid_slots = (slot_ids < mask_count[:, None]).astype(F32)
    patch_ids = lax.broadcasted_iota(jnp.int32, (1, 1, seq_len), 2)
    onehot = (mask_index[:, :, None] == patch_ids).astype(F32)
    return jnp.einsum("cj,cjp->cp", valid_slots, onehot).reshape(-1, 1)


def kernel_layer(patches, cotangent, mask_index, mask_count, *shards):
    masked = mask_rows(mask_index, mask_count, 512)
    rows = jnp.pad(jnp.stack([shards[i] for i in SMALL]), ((0, 0), (0, 32)))
    small = jnp.pad(jnp.concatenate([rows, shards[11].reshape(3, 128)]), ((0, 4), (0, 0)))
    results = forward_call(patches.reshape(1024, 768), masked, *[shards[i] for i in BIG], small)
    full, kept = results[:4], results[4:]
    held = (cotangent.reshape(1024, 768),) + tuple(kept[:10])
    *blocks, total, patch_grad = backward_call(kept[11], masked, held, full)
    mine, bias_fc1 = place_small(total)
    grads = [None] * 14
    for row, i in enumerate(SMALL):
        grads[i] = mine[row]
    for i, block in zip(BIG, blocks):
        grads[i] = block
    grads[11] = bias_fc1
    return (kept[10].reshape(patches.shape), patch_grad.reshape(patches.shape)) + tuple(grads)


def plain_layer(patches, cotangent, mask_index, mask_count, *shards):
    output, patch_grad, grads = compute(patches, cotangent, mask_index, mask_count, plain_gather(shards))
    return (output, patch_grad) + plain_reduce(grads)


def solution(mesh):
    in_specs = (
        P(("narrow", "wide"), None, None),
        P(("narrow", "wide"), None, None),
        P(("narrow", "wide"), None),
        P(("narrow", "wide")),
        P("wide"),
        P("wide"),
        P("wide"),
        P("wide", None),
        P("wide"),
        P("wide"),
        P("wide", None),
        P("wide"),
        P("wide"),
        P("wide"),
        P("wide", None),
        P("wide"),
        P("wide", None),
        P("wide"),
    )
    out_specs = (
        P(("narrow", "wide"), None, None),
        P(("narrow", "wide"), None, None),
        P("wide"),
        P("wide"),
        P("wide"),
        P("wide", None),
        P("wide"),
        P("wide"),
        P("wide", None),
        P("wide"),
        P("wide"),
        P("wide"),
        P("wide", None),
        P("wide"),
        P("wide", None),
        P("wide"),
    )
    kernels = mesh.shape["narrow"] == 4 and mesh.shape["wide"] == 8
    return jax.shard_map(
        kernel_layer if kernels else plain_layer, mesh=mesh, in_specs=in_specs, out_specs=out_specs, check_vma=False
    )
```

```python
import jax
import jax.numpy as jnp
from jax import lax
from jax.experimental import pallas as pl
from jax.experimental.pallas import tpu as pltpu
from jax.sharding import PartitionSpec as P

HEADS = 12
HD = 64


epsilon = 1e-06
inv_root_two = 0.7071067811865476
inv_root_tau = 0.3989422804014327


def dot_rows(left_side, right_side):
    return lax.dot_general(
        left_side, right_side, (((0,), (0,)), ((), ())), preferred_element_type=jnp.float32
    )


def dot_back(left_side, right_side):
    return lax.dot_general(
        left_side, right_side, (((1,), (1,)), ((), ())), preferred_element_type=jnp.float32
    )


def norm_rows(values):
    row_mean = jnp.mean(values, axis=-1, keepdims=True)
    centered = values - row_mean
    variance = jnp.mean(centered * centered, axis=-1, keepdims=True)
    inv_std = lax.rsqrt(variance + epsilon)
    return (centered * inv_std, inv_std)


def norm_back(grad_in, normed, inv_std, ln_gain):
    grad_normed = grad_in * ln_gain[None, :]
    mean_grad = jnp.mean(grad_normed, axis=-1, keepdims=True)
    mean_cross = jnp.mean(grad_normed * normed, axis=-1, keepdims=True)
    return inv_std * (grad_normed - mean_grad - normed * mean_cross)


def split_heads(qkv_clip):
    seq_len = qkv_clip.shape[0]
    split_qkv = qkv_clip.reshape(seq_len, 3, HEADS, HD)
    return (split_qkv[:, 0], split_qkv[:, 1], split_qkv[:, 2])


def clip_scores(query_rows, key_rows):
    return jnp.einsum(
        "qhd,khd->hqk", query_rows, key_rows, preferred_element_type=jnp.float32
    ) * HD ** (-0.5)


def attend(qkv_clip):
    query_rows, key_rows, value_rows = split_heads(qkv_clip)
    scores = clip_scores(query_rows, key_rows)
    row_max = jnp.max(scores, axis=-1, keepdims=True)
    exp_scores = jnp.exp(scores - row_max)
    row_total = jnp.sum(exp_scores, axis=-1, keepdims=True)
    soft_probs = (exp_scores / row_total).astype(jnp.bfloat16)
    attn_mixed = jnp.einsum(
        "hqk,khd->qhd", soft_probs, value_rows, preferred_element_type=jnp.float32
    )
    log_total = (row_max + jnp.log(row_total))[..., 0]
    return (attn_mixed.reshape(qkv_clip.shape[0], HEADS * HD).astype(jnp.bfloat16), log_total)


def attend_back(block_args):
    qkv_clip, grad_mixed, log_total = block_args
    query_rows, key_rows, value_rows = split_heads(qkv_clip)
    grad_heads = grad_mixed.reshape(qkv_clip.shape[0], HEADS, HD)
    soft_probs = jnp.exp(clip_scores(query_rows, key_rows) - log_total[..., None])
    grad_probs = jnp.einsum(
        "qhd,khd->hqk", grad_heads, value_rows, preferred_element_type=jnp.float32
    )
    grad_value = jnp.einsum(
        "hqk,qhd->khd",
        soft_probs.astype(jnp.bfloat16),
        grad_heads,
        preferred_element_type=jnp.float32,
    )
    grad_scores = soft_probs * (
        grad_probs - jnp.sum(soft_probs * grad_probs, axis=-1, keepdims=True)
    )
    grad_scores = grad_scores.astype(jnp.bfloat16)
    grad_query = jnp.einsum(
        "hqk,khd->qhd", grad_scores, key_rows, preferred_element_type=jnp.float32
    ) * HD ** (-0.5)
    grad_key = jnp.einsum(
        "hqk,qhd->khd", grad_scores, query_rows, preferred_element_type=jnp.float32
    ) * HD ** (-0.5)
    stacked = jnp.stack([grad_query, grad_key, grad_value], axis=1)
    return stacked.reshape(qkv_clip.shape[0], 3 * HEADS * HD).astype(jnp.bfloat16)


MESH = pl.DeviceIdType.MESH
BF = jnp.bfloat16
F32 = jnp.float32

UNITS = (
    [("qkv", 768 * j, 0) for j in range(3)]
    + [("out", 0, 0)]
    + [("fc1", 768 * j, 0) for j in range(4)]
    + [("fc2", 0, 96 * j) for j in range(4)]
)
NU = len(UNITS)


def lanes(start):
    return pl.multiple_of(start, 128)


class Place:
    def __init__(self):
        n = lax.axis_index("narrow")
        w = lax.axis_index("wide")
        self.n, self.w = n, w
        self.core, self.x = n % 2, n // 2
        self.y, self.z = w % 2, w // 2
        self.core_peer = (self.x * 2 + (1 - self.core), w)
        self.x_peer = ((1 - self.x) * 2 + self.core, w)
        self.y_peer = (n, self.z * 2 + (1 - self.y))

    def z_up(self, k):
        return (self.z + k) % 4

    def z_peer(self, k):
        return (self.n, self.z_up(k) * 2 + self.y)

    def greet(self):
        barrier = pltpu.get_barrier_semaphore()
        peers = [self.core_peer, self.x_peer, self.y_peer] + [self.z_peer(k) for k in (1, 2, 3)]
        for peer in peers:
            pl.semaphore_signal(barrier, inc=1, device_id=peer, device_id_type=MESH)
        pl.semaphore_wait(barrier, len(peers))


def remote(src, dst, send, recv, peer):
    return pltpu.make_async_remote_copy(
        src_ref=src, dst_ref=dst, send_sem=send, recv_sem=recv, device_id=peer, device_id_type=MESH
    )


class Gather:
    SEMS = [
        pltpu.SemaphoreType.DMA((NU, 10)),
        pltpu.SemaphoreType.DMA((NU, 10)),
        pltpu.SemaphoreType.DMA((NU,)),
        pltpu.SemaphoreType.DMA((8,)),
        pltpu.SemaphoreType.DMA((8,)),
    ]

    def __init__(self, place, shards, full, small, small_full, send, recv, local, ssend, srecv):
        self.p, self.shards, self.full = place, shards, full
        self.small, self.small_full = small, small_full
        self.send, self.recv, self.local, self.ssend, self.srecv = send, recv, local, ssend, srecv
        self.sent = []

    def go(self, u, i, src, dst, peer):
        copy = remote(src, dst, self.send.at[u, i], self.recv.at[u, i], peer)
        copy.start()
        self.sent.append(copy)

    def arrived(self, u, i, dst):
        remote(dst, dst, self.send.at[u, i], self.recv.at[u, i], self.p.x_peer).wait_recv()

    def small_stage(self, stage):
        p = self.p
        if stage == 0:
            own = self.small_full.at[p.z, p.y]
            pltpu.make_async_copy(self.small, own, self.local.at[0]).start()
            pltpu.make_async_copy(self.small, own, self.local.at[0]).wait()
            for k in (1, 2, 3):
                copy = remote(self.small, own, self.ssend.at[k], self.srecv.at[k], p.z_peer(k))
                copy.start()
                self.sent.append(copy)
        elif stage == 1:
            for k in (1, 2, 3):
                dst = self.small_full.at[p.z_up(4 - k), p.y]
                remote(dst, dst, self.ssend.at[k], self.srecv.at[k], p.x_peer).wait_recv()
            mine = self.small_full.at[:, p.y]
            copy = remote(mine, mine, self.ssend.at[0], self.srecv.at[0], p.y_peer)
            copy.start()
            self.sent.append(copy)
        else:
            dst = self.small_full.at[:, 1 - p.y]
            remote(dst, dst, self.ssend.at[0], self.srecv.at[0], p.x_peer).wait_recv()

    def stage(self, u, stage):
        p = self.p
        name, co, ro = UNITS[u]
        full, shard = self.full[name], self.shards[name]
        rows = pl.ds(ro, 96)
        own = pl.ds(lanes(co + p.core * 384 + p.x * 128), 256)
        exc = pl.ds(lanes(co + p.core * 384 + p.x * 256), 128)
        peer_exc = pl.ds(lanes(co + p.core * 384 + (1 - p.x) * 256), 128)
        oth = pl.ds(lanes(co + (1 - p.core) * 384 + p.x * 128), 256)
        oth_exc = pl.ds(lanes(co + (1 - p.core) * 384 + (1 - p.x) * 256), 128)
        if stage == 0:
            mine = shard.at[rows, own]
            home = full.at[p.z, p.y, rows, own]
            pltpu.make_async_copy(mine, home, self.local.at[u]).start()
            for k in (1, 2, 3):
                self.go(u, k, mine, home, p.z_peer(k))
        elif stage == 1:
            home = full.at[p.z, p.y, rows, own]
            pltpu.make_async_copy(shard.at[rows, own], home, self.local.at[u]).wait()
            for k in (1, 2, 3):
                self.arrived(u, k, full.at[p.z_up(4 - k), p.y, rows, own])
            column = full.at[:, p.y, rows, own]
            part = full.at[:, p.y, rows, exc]
            self.go(u, 0, column, column, p.y_peer)
            self.go(u, 4, part, part, p.x_peer)
            self.go(u, 5, column, column, p.core_peer)
        elif stage == 2:
            column = full.at[:, 1 - p.y, rows, own]
            part = full.at[:, 1 - p.y, rows, exc]
            self.arrived(u, 0, column)
            self.go(u, 6, part, part, p.x_peer)
            self.go(u, 7, column, column, p.core_peer)
        elif stage == 3:
            self.arrived(u, 4, full.at[:, p.y, rows, peer_exc])
            self.arrived(u, 6, full.at[:, 1 - p.y, rows, peer_exc])
            both = full.at[:, :, rows, peer_exc]
            self.go(u, 8, both, both, p.core_peer)
        else:
            self.arrived(u, 5, full.at[:, p.y, rows, oth])
            self.arrived(u, 7, full.at[:, 1 - p.y, rows, oth])
            self.arrived(u, 8, full.at[:, :, rows, oth_exc])

    def finish(self):
        for copy in self.sent:
            copy.wait_send()


class Reduce:
    SCRATCH = [
        pltpu.VMEM((NU, 4, 2, 96, 384), BF),
        pltpu.VMEM((NU, 4, 2, 96, 128), BF),
        pltpu.VMEM((NU, 4, 96, 256), BF),
        pltpu.VMEM((NU, 3, 96, 256), BF),
        pltpu.VMEM((NU, 2, 96, 256), BF),
        pltpu.VMEM((NU, 2, 96, 384), BF),
        pltpu.VMEM((10, 16, 768), F32),
        pltpu.SemaphoreType.DMA((NU, 8)),
        pltpu.SemaphoreType.DMA((NU, 8)),
        pltpu.SemaphoreType.DMA((6,)),
        pltpu.SemaphoreType.DMA((6,)),
    ]

    def __init__(self, place, grads, outs, staging, out_sem, bufs):
        self.p, self.grads, self.outs = place, grads, outs
        self.staging, self.out_sem, self.leaving = staging, out_sem, []
        (self.c, self.xb, self.yb, self.zb, self.f, self.e, self.s,
         self.send, self.recv, self.ssend, self.srecv) = bufs
        self.sent = []

    def go(self, u, i, src, dst, peer):
        copy = remote(src, dst, self.send.at[u, i], self.recv.at[u, i], peer)
        copy.start()
        self.sent.append(copy)

    def arrived(self, u, i, dst):
        remote(dst, dst, self.send.at[u, i], self.recv.at[u, i], self.p.x_peer).wait_recv()

    def stage(self, u, stage):
        p = self.p
        name, co, ro = RUNITS[u]
        grad = self.grads[name]
        rows = pl.ds(ro, 96)
        own = pl.ds(lanes(co + p.core * 384), 384)
        oth = pl.ds(lanes(co + (1 - p.core) * 384), 384)
        exc = pl.ds(lanes(p.x * 256), 128)
        peer_exc = pl.ds(lanes((1 - p.x) * 256), 128)
        two = pl.ds(lanes(p.x * 128), 256)
        c, xb, yb, zb = self.c.at[u], self.xb.at[u], self.yb.at[u], self.zb.at[u]
        if stage == 0:
            self.go(u, 0, grad.at[:, :, rows, oth], c, p.core_peer)
        elif stage == 1:
            self.arrived(u, 0, c)

            def add(i, carry):
                a, b = i // 2, i % 2
                c[a, b] = c[a, b] + grad[a, b, rows, own]
                return carry

            lax.fori_loop(0, 8, add, 0)
            self.go(u, 1, c.at[:, :, :, peer_exc], xb, p.x_peer)
        elif stage == 2:
            self.arrived(u, 1, xb)

            def add(i, carry):
                a, b = i // 2, i % 2
                c[a, b, :, exc] = c[a, b, :, exc] + xb[a, b]
                return carry

            lax.fori_loop(0, 8, add, 0)
            self.go(u, 2, c.at[:, 1 - p.y, :, two], yb, p.y_peer)
        elif stage == 3:
            self.arrived(u, 2, yb)

            def add(a, carry):
                c[a, p.y, :, two] = c[a, p.y, :, two] + yb[a]
                return carry

            lax.fori_loop(0, 4, add, 0)
            for k in (1, 2, 3):
                self.go(u, 2 + k, c.at[p.z_up(k), p.y, :, two], zb.at[k - 1], p.z_peer(k))
        elif stage == 4:
            for k in (1, 2, 3):
                self.arrived(u, 2 + k, zb.at[k - 1])
            total = c[p.z, p.y, :, two].astype(F32)
            for k in (1, 2, 3):
                total = total + zb[k - 1].astype(F32)
            self.f[u, 0] = total.astype(BF)
            self.go(u, 6, self.f.at[u, 0], self.f.at[u, 1], p.x_peer)
        elif stage == 5:
            self.arrived(u, 6, self.f.at[u, 1])
            low = self.f[u, p.x].astype(F32)
            high = self.f[u, 1 - p.x].astype(F32)
            self.e[u, 0, :, 0:128] = low[:, 0:128].astype(BF)
            self.e[u, 0, :, 128:256] = (low[:, 128:] + high[:, :128]).astype(BF)
            self.e[u, 0, :, 256:384] = high[:, 128:].astype(BF)
            self.go(u, 7, self.e.at[u, 0], self.e.at[u, 1], p.core_peer)
        else:
            self.arrived(u, 7, self.e.at[u, 1])
            slot = self.staging.at[u % 3]
            if u >= 3:
                for copy in self.leaving[u - 3]:
                    copy.wait()
            slot[:, pl.ds(lanes(p.core * 384), 384)] = self.e[u, 0]
            slot[:, pl.ds(lanes((1 - p.core) * 384), 384)] = self.e[u, 1]
            pieces = []
            for q in range(3):
                start = co // 3 + 768 * q if name == "qkv" else co + 256 * q
                target = self.outs[name].at[rows, pl.ds(start, 256)]
                copy = pltpu.make_async_copy(slot.at[:, pl.ds(256 * q, 256)], target, self.out_sem.at[u, q])
                copy.start()
                pieces.append(copy)
            self.leaving.append(pieces)

    def small_stage(self, stage, mine=None):
        p, s = self.p, self.s
        peers = [p.core_peer, p.x_peer, p.y_peer]
        if stage == 0:
            s[0] = mine
        elif stage <= 3:
            i = stage - 1
            dst = s.at[2 * i + 1]
            remote(dst, dst, self.ssend.at[i], self.srecv.at[i], p.x_peer).wait_recv()
            s[2 * i + 2] = s[2 * i] + s[2 * i + 1]
        if stage < 3:
            copy = remote(s.at[2 * stage], s.at[2 * stage + 1], self.ssend.at[stage], self.srecv.at[stage], peers[stage])
            copy.start()
            self.sent.append(copy)
        elif stage == 3:
            for k in (1, 2, 3):
                copy = remote(s.at[6], s.at[6 + k], self.ssend.at[2 + k], self.srecv.at[2 + k], p.z_peer(k))
                copy.start()
                self.sent.append(copy)
        else:
            total = s[6]
            for k in (1, 2, 3):
                dst = s.at[6 + k]
                remote(dst, dst, self.ssend.at[2 + k], self.srecv.at[2 + k], p.x_peer).wait_recv()
                total = total + s[6 + k]
            return total

    def finish(self):
        for copy in self.sent:
            copy.wait_send()
        for pieces in self.leaving[-3:]:
            for copy in pieces:
                copy.wait()


def kernel_params(cid, side=True):
    return pltpu.CompilerParams(collective_id=cid, has_side_effects=side, vmem_limit_bytes=67043328)


VM = pl.BlockSpec(memory_space=pltpu.VMEM)
ANY = pl.BlockSpec(memory_space=pl.ANY)
NAMES = ("qkv", "out", "fc1", "fc2")
FULL = {"qkv": (4, 2, 96, 2304), "out": (4, 2, 96, 768), "fc1": (4, 2, 96, 3072), "fc2": (4, 2, 384, 768)}


def row_block(i, size):
    return pl.ds(pl.multiple_of(i * size, size), size)


class Ticks:
    def __init__(self, run, stages, ahead):
        self.run, self.stages, self.ahead = run, stages, ahead
        self.t = 0
        for u in range(ahead):
            run(u, 0)

    def tick(self):
        t = self.t
        self.t += 1
        if t + self.ahead < NU:
            self.run(t + self.ahead, 0)
        for s in range(1, self.stages):
            if 0 <= t - s + 1 < NU:
                self.run(t - s + 1, s)

    def need(self, u):
        while self.t < u + self.stages - 1:
            self.tick()


def matmul(left, right):
    return jnp.dot(left, right, preferred_element_type=F32)


def norm_block(values):
    mean = jnp.mean(values, axis=1, keepdims=True)
    centered = values - mean
    variance = jnp.mean(centered * centered, axis=1, keepdims=True)
    inv_std = lax.rsqrt(variance + epsilon)
    return centered * inv_std, inv_std


KEPT = (
    ("attn_in", (1024, 768), BF),
    ("normed1", (1024, 768), BF),
    ("rstd1", (1024, 128), F32),
    ("qkv", (1024, 2304), BF),
    ("mixed", (1024, 768), BF),
    ("mlp_in", (1024, 768), BF),
    ("normed2", (1024, 768), BF),
    ("rstd2", (1024, 128), F32),
    ("slope", (1024, 3072), BF),
    ("g_fc2", (4, 2, 384, 768), BF),
    ("out", (1024, 768), BF),
    ("vec", (16, 768), F32),
)


def attend_pair(qkv, mixed, i):
    clip, pair = i // 6, i % 6
    rows = row_block(clip, 512)
    at = pl.multiple_of(pair * 128, 128)
    q2 = qkv[rows, pl.ds(at, 128)]
    k2 = qkv[rows, pl.ds(pl.multiple_of(at + 768, 128), 128)]
    v2 = qkv[rows, pl.ds(pl.multiple_of(at + 1536, 128), 128)]
    lane = lax.broadcasted_iota(jnp.int32, (512, 128), 1)
    parts = []
    for h in range(2):
        inside = (lane >= 64) if h else (lane < 64)
        qh = jnp.where(inside, q2 * jnp.asarray(0.125, BF), jnp.zeros_like(q2))
        scores = lax.dot_general(qh, k2, (((1,), (1,)), ((), ())), preferred_element_type=F32)
        e = jnp.exp(scores - jnp.max(scores, axis=1, keepdims=True))
        total = jnp.sum(e, axis=1, keepdims=True)
        parts.append(matmul(e.astype(BF), v2) * (1.0 / total))
    mixed[rows, pl.ds(at, 128)] = jnp.where(lane < 64, parts[0], parts[1]).astype(BF)


def forward_kernel(*refs):
    patches, mask, cot = refs[0:3]
    shards = dict(zip(NAMES, refs[3:7]))
    small = refs[7]
    n_out = 4 + len(KEPT)
    full_out = dict(zip(NAMES, refs[8:12]))
    kept_out = dict(zip([k[0] for k in KEPT], refs[12 : 8 + n_out]))
    rest = refs[8 + n_out :]
    full = dict(zip(NAMES, rest[0:4]))
    kept = dict(zip([k[0] for k in KEPT], rest[4 : 4 + len(KEPT)]))
    middle, small_full, bias1, act, out_sem = rest[4 + len(KEPT) : 9 + len(KEPT)]
    sems = rest[9 + len(KEPT) :]
    place = Place()
    place.greet()
    g = Gather(place, shards, full, small, small_full, *sems)
    leaving = []

    def leave(src, dst):
        copy = pltpu.make_async_copy(src, dst, out_sem.at[len(leaving)])
        copy.start()
        leaving.append(copy)

    def keep(name):
        leave(kept[name], kept_out[name])

    g.small_stage(0)
    ticks = Ticks(g.stage, 5, 2)
    g.small_stage(1)
    g.small_stage(2)
    ticks.tick()
    vec = kept["vec"]
    total = jnp.zeros((16, 768), F32)
    spot = lax.broadcasted_iota(jnp.int32, (128, 768), 1) - lax.broadcasted_iota(jnp.int32, (128, 768), 0)
    inside = lax.broadcasted_iota(jnp.int32, (128, 768), 0) < 96
    for s in range(8):
        block = small_full[s // 2, s % 2]
        pick = jnp.where((spot == 96 * s) & inside, 1.0, 0.0).astype(BF)
        total = total + matmul(block, pick)
        wide = block.astype(F32)
        for r in range(3):
            bias1[:, pl.ds(s * 384 + r * 128, 128)] = jnp.broadcast_to(wide[9 + r : 10 + r, :], (8, 128))
    vec[...] = total
    keep("vec")

    def norm1(i, carry):
        rows = row_block(i, 128)
        m = mask[rows, 0:1]
        start = patches[rows, :].astype(F32) * (1.0 - m) + m * vec[0:1, :]
        normed, inv_std = norm_block(start)
        middle[rows, :] = start
        kept["normed1"][rows, :] = normed.astype(BF)
        kept["rstd1"][rows, :] = jnp.broadcast_to(inv_std, (128, 128))
        kept["attn_in"][rows, :] = (normed * vec[1:2, :] + vec[2:3, :]).astype(BF)
        return carry

    lax.fori_loop(0, 4, norm1, 0)
    ticks.tick()
    lax.fori_loop(4, 8, norm1, 0)
    ticks.tick()
    for name in ("attn_in", "normed1", "rstd1"):
        keep(name)
    for u in range(3):
        ticks.need(u)
        w = full["qkv"][:, :, :, pl.ds(768 * u, 768)].reshape(768, 768)

        def project(i, carry):
            rows = row_block(i, 256)
            value = matmul(kept["attn_in"][rows, :], w)
            if u != 1:
                row = 3 if u == 0 else 4
                value = value + vec[row : row + 1, :]
            kept["qkv"][rows, pl.ds(768 * u, 768)] = value.astype(BF)
            return carry

        lax.fori_loop(0, 4, project, 0)
    leave(full["qkv"], full_out["qkv"])
    keep("qkv")
    for part in range(3):

        def attend_four(i, carry):
            attend_pair(kept["qkv"], kept["mixed"], i)
            return carry

        lax.fori_loop(4 * part, 4 * part + 4, attend_four, 0)
        ticks.tick()
    keep("mixed")
    ticks.need(3)
    leave(full["out"], full_out["out"])
    w_out = full["out"][...].reshape(768, 768)

    def mix(i, carry):
        rows = row_block(i, 512)
        middle[rows, :] = middle[rows, :] + (matmul(kept["mixed"][rows, :], w_out) + vec[5:6, :])
        return carry

    lax.fori_loop(0, 2, mix, 0)
    ticks.tick()

    def norm2(i, carry):
        rows = row_block(i, 128)
        normed, inv_std = norm_block(middle[rows, :])
        kept["normed2"][rows, :] = normed.astype(BF)
        kept["rstd2"][rows, :] = jnp.broadcast_to(inv_std, (128, 128))
        kept["mlp_in"][rows, :] = (normed * vec[6:7, :] + vec[7:8, :]).astype(BF)
        return carry

    lax.fori_loop(0, 8, norm2, 0)
    for name in ("normed2", "rstd2", "mlp_in"):
        keep(name)
    for j in range(4):
        ticks.need(4 + j)
        w = full["fc1"][:, :, :, pl.ds(768 * j, 768)].reshape(768, 768)

        def expand(i, carry):
            rows = row_block(i, 256)
            cols = pl.ds(768 * j, 768)
            h = matmul(kept["mlp_in"][rows, :], w) + bias1[0:1, cols]
            below = 0.5 * (1.0 + lax.erf(h * inv_root_two))
            density = jnp.exp(-0.5 * h * h) * inv_root_tau
            act[rows, cols] = (h * below).astype(BF)
            kept["slope"][rows, cols] = (below + h * density).astype(BF)
            return carry

        lax.fori_loop(0, 4, expand, 0)
        ticks.tick()

        def weight_fc2(y, carry):
            left = act[:, pl.ds(pl.multiple_of(768 * j + y * 384, 128), 384)]
            kept["g_fc2"][j, y] = dot_rows(left, cot[...]).astype(BF)
            return carry

        lax.fori_loop(0, 2, weight_fc2, 0)
    leave(full["fc1"], full_out["fc1"])
    keep("slope")
    keep("g_fc2")
    ticks.need(NU - 1)
    leave(full["fc2"], full_out["fc2"])

    def contract(i, carry):
        rows = row_block(i, 256)
        value = middle[rows, :] + vec[8:9, :]
        for k in range(4):
            w = full["fc2"][k].reshape(768, 768)
            value = value + matmul(act[rows, pl.ds(768 * k, 768)], w)
        kept["out"][rows, :] = value.astype(BF)
        return carry

    lax.fori_loop(0, 4, contract, 0)
    keep("out")
    g.finish()
    for copy in leaving:
        copy.wait()


def forward_call(patches, mask, cot, qkv, out, fc1, fc2, small):
    shapes = [jax.ShapeDtypeStruct(FULL[k], BF) for k in NAMES]
    shapes += [jax.ShapeDtypeStruct(k[1], k[2]) for k in KEPT]
    scratch = [pltpu.VMEM(FULL[k], BF) for k in NAMES]
    scratch += [pltpu.VMEM(k[1], k[2]) for k in KEPT]
    scratch += [
        pltpu.VMEM((1024, 768), F32),
        pltpu.VMEM((4, 2, 16, 128), BF),
        pltpu.VMEM((8, 3072), F32),
        pltpu.VMEM((1024, 3072), BF),
        pltpu.SemaphoreType.DMA((4 + len(KEPT),)),
    ]
    return pl.pallas_call(
        forward_kernel,
        out_shape=shapes,
        in_specs=[VM] * 8,
        out_specs=[ANY] * len(shapes),
        scratch_shapes=scratch + Gather.SEMS,
        compiler_params=kernel_params(0),
        name="forward",
    )(patches, mask, cot, qkv, out, fc1, fc2, small)

RUNITS = UNITS[8:12] + UNITS[4:8] + UNITS[3:4] + UNITS[0:3]


class Service:
    def __init__(self, run, stages):
        self.run, self.stages = run, stages
        self.ready, self.at = 0, []

    def call(self):
        if len(self.at) < self.ready:
            self.at.append(0)
        for u in reversed(range(len(self.at))):
            if self.at[u] < self.stages:
                self.run(u, self.at[u])
                self.at[u] += 1

    def busy(self):
        return len(self.at) < self.ready or any(a < self.stages for a in self.at)


def attend_pair_back(qkv, mixed, grad_mixed, grad_qkv, sums, acc, i):
    pair, clip = i // 2, i % 2
    rows = row_block(clip, 512)
    at = pl.multiple_of(pair * 128, 128)
    spots = [pl.ds(pl.multiple_of(at + 768 * p, 128), 128) for p in range(3)]
    group = (pair // 2) * 768 + (pair % 2) * 128
    eighth = jnp.asarray(0.125, BF)
    acc[...] = jnp.zeros_like(acc)

    def part(block, carry):
        q_rows = pl.ds(pl.multiple_of(clip * 512 + block * 256, 256), 256)
        own = pl.ds(pl.multiple_of(block * 256, 256), 256)
        lane = lax.broadcasted_iota(jnp.int32, (256, 128), 1)
        lane_keys = lax.broadcasted_iota(jnp.int32, (512, 128), 1)
        q2 = qkv[q_rows, spots[0]]
        k2 = qkv[rows, spots[1]]
        v2 = qkv[rows, spots[2]]
        grad2 = grad_mixed[q_rows, pl.ds(at, 128)]
        product = grad2.astype(F32) * mixed[q_rows, pl.ds(at, 128)].astype(F32)
        grads = [0.0, 0.0, 0.0]
        for head in range(2):
            inside = (lane >= 64) if head else (lane < 64)
            inside_keys = (lane_keys >= 64) if head else (lane_keys < 64)
            free = 0 if head else 64
            qh = jnp.where(inside, q2 * eighth, jnp.zeros_like(q2))
            kh = jnp.where(inside_keys, k2 * eighth, jnp.zeros_like(k2))
            gh = jnp.where(inside, grad2, jnp.zeros_like(grad2))
            shared = jnp.sum(jnp.where(inside, product, 0.0), axis=1, keepdims=True)
            first = shared.astype(BF).astype(F32)
            second = (shared - first).astype(BF).astype(F32)
            third = shared - first - second
            extra = jnp.where(lane == free, first, jnp.where(lane == free + 1, second, third))
            taken = (lane >= free) & (lane < free + 3)
            g_less = jnp.where(inside, grad2, jnp.where(taken, extra, 0.0).astype(BF))
            taken_keys = (lane_keys >= free) & (lane_keys < free + 3)
            v_less = jnp.where(inside_keys, v2, jnp.where(taken_keys, -1.0, 0.0).astype(BF))
            scores = dot_back(k2, qh)
            e = jnp.exp(scores - jnp.max(scores, axis=0, keepdims=True))
            probs = e * (1.0 / jnp.sum(e, axis=0, keepdims=True))
            grad_scores = (probs * dot_back(v_less, g_less)).astype(BF)
            grads[2] = grads[2] + matmul(probs.astype(BF), gh)
            grads[1] = grads[1] + matmul(grad_scores, qh)
            grads[0] = grads[0] + dot_rows(grad_scores, kh)
        acc[2] += grads[2]
        acc[1] += grads[1]
        acc[0, own, :] = grads[0]
        return carry

    lax.fori_loop(0, 2, part, 0)
    for p in range(3):
        value = acc[p].astype(BF)
        grad_qkv[rows, pl.ds(pl.multiple_of(group + 256 * p, 128), 128)] = value
        if p != 1:
            row = 3 if p == 0 else 4
            sums[row : row + 1, pl.ds(at, 128)] += jnp.sum(value.astype(F32), axis=0, keepdims=True)


def backward_kernel(*refs):
    vec, mask = refs[0:2]
    names = ("cot", "attn_in", "normed1", "rstd1", "qkv", "mixed", "mlp_in", "normed2", "rstd2", "slope", "g_fc2")
    held = dict(zip(names, refs[2:13]))
    weights = dict(zip(NAMES, refs[13:17]))
    outs = dict(zip(NAMES, refs[17:21]))
    small_out, patch_out = refs[21:23]
    (cot, act, slope, w2, w1, mlp_in, normed2, rstd2, mixed, total, sums, acc,
     g_fc2, g_fc1, g_out, staging, load_sem, out_sem) = refs[23:41]
    place = Place()
    place.greet()
    grads = {"qkv": w1, "out": g_out, "fc1": g_fc1, "fc2": g_fc2}
    r = Reduce(place, grads, outs, staging, out_sem, refs[41:])
    svc = Service(r.stage, 7)
    loads = {}

    def load(name, src, dst):
        copy = pltpu.make_async_copy(src, dst, load_sem.at[len(loads)])
        copy.start()
        loads[name] = copy

    def loaded(*names):
        for name in names:
            loads[name].wait()

    load("g_fc2", held["g_fc2"], g_fc2)
    load("cot", held["cot"], cot)
    load("fc2", weights["fc2"], w2)
    load("slope", held["slope"], slope)
    load("mlp_in", held["mlp_in"], mlp_in)
    load("fc1", weights["fc1"], w1)
    load("normed2", held["normed2"], normed2)
    load("rstd2", held["rstd2"], rstd2)
    load("mixed", held["mixed"], mixed)
    sums[...] = jnp.zeros_like(sums)
    loaded("g_fc2")
    svc.ready = 4
    svc.call()
    loaded("cot")

    def bias_fc2(i, carry):
        sums[8:9, :] += jnp.sum(cot[row_block(i, 256), :].astype(F32), axis=0, keepdims=True)
        return carry

    lax.fori_loop(0, 4, bias_fc2, 0)
    loaded("fc2", "slope", "mlp_in", "fc1")

    def weight_grad(left, right, target):
        def some(i, carry):
            rows = left[:, pl.ds(pl.multiple_of(i * 384, 128), 384)]
            value = dot_rows(rows, right()).astype(BF).reshape(2, 2, 96, 768)
            target(pl.ds(2 * i, 2), value)
            return carry

        lax.fori_loop(0, 2, some, 0)

    for j in range(4):
        cols = pl.ds(768 * j, 768)

        def hidden(i, carry):
            rows = row_block(i, 256)
            value = dot_back(cot[rows, :], w2[j].reshape(768, 768)) * slope[rows, cols].astype(F32)
            value = value.astype(BF)
            slope[rows, cols] = value
            sums[9 + j : 10 + j, :] += jnp.sum(value.astype(F32), axis=0, keepdims=True)
            return carry

        lax.fori_loop(0, 4, hidden, 0)
        if j % 2:
            svc.call()
        if j == 3:
            for n in range(3):
                for p in range(3):
                    source = weights["qkv"].at[:, :, :, pl.ds(768 * p + 256 * n, 256)]
                    load(f"w{n}{p}", source, w2.at[:, :, pl.ds(96 * n, 96), pl.ds(256 * p, 256)])
            load("w3", weights["out"], w2.at[:, :, pl.ds(288, 96), :])

        def put_fc1(z, value):
            g_fc1[z, :, :, cols] = value

        weight_grad(mlp_in, lambda: slope[:, cols], put_fc1)
        svc.ready = 5 + j

        def spread(i, carry):
            rows = row_block(i, 256)
            value = dot_back(slope[rows, cols], w1[:, :, :, cols].reshape(768, 768))
            total[rows, :] = value if j == 0 else total[rows, :] + value
            return carry

        lax.fori_loop(0, 4, spread, 0)
        svc.call()
    load("qkv", held["qkv"], slope.at[:, pl.ds(0, 2304)])
    loaded("normed2", "rstd2")

    def norm_step(grad, normed, inv_std, gain):
        scaled = grad * gain
        mean = jnp.mean(scaled, axis=1, keepdims=True)
        cross = jnp.mean(scaled * normed, axis=1, keepdims=True)
        return inv_std * (scaled - mean - normed * cross)

    def column_sum(row, value):
        sums[row : row + 1, :] += jnp.sum(value, axis=0, keepdims=True)

    def norm2(i, carry):
        rows = row_block(i, 128)
        grad, normed = total[rows, :], normed2[rows, :].astype(F32)
        column_sum(6, grad * normed)
        column_sum(7, grad)
        middle = cot[rows, :].astype(F32) + norm_step(grad, normed, rstd2[rows, 0:1], vec[6:7, :])
        total[rows, :] = middle
        branch = middle.astype(BF)
        mlp_in[rows, :] = branch
        column_sum(5, branch.astype(F32))
        return carry

    lax.fori_loop(0, 8, norm2, 0)
    load("normed1", held["normed1"], normed2)
    load("rstd1", held["rstd1"], rstd2)
    loaded("mixed", "w3")

    def put_out(z, value):
        g_out[z] = value

    weight_grad(mixed, lambda: mlp_in[...], put_out)
    svc.ready = 9

    def branch_back(i, carry):
        rows = row_block(i, 512)
        w = w2[:, :, pl.ds(288, 96), :].reshape(768, 768)
        cot[rows, :] = dot_back(mlp_in[rows, :], w).astype(BF)
        return carry

    lax.fori_loop(0, 2, branch_back, 0)
    svc.call()
    load("attn_in", held["attn_in"], mlp_in)
    loaded("qkv")
    loaded("attn_in")
    for n in range(3):

        def attend_four(i, carry):
            attend_pair_back(slope, mixed, cot, act, sums, acc, i)
            return carry

        lax.fori_loop(4 * n, 4 * n + 4, attend_four, 0)
        svc.call()
        cols = pl.ds(768 * n, 768)

        def put_qkv(z, value):
            w1[z, :, :, cols] = value

        weight_grad(mlp_in, lambda: act[:, cols], put_qkv)
        svc.ready = 10 + n
        svc.call()
    loaded("normed1", "rstd1", *[f"w{n}{p}" for n in range(3) for p in range(3)])

    def norm1(i, carry):
        rows = row_block(i, 256)
        grad = jnp.zeros((256, 768), F32)
        for p in range(3):
            w = w2[:, :, pl.ds(96 * p, 96), :].reshape(768, 768)
            grad = grad + dot_back(act[rows, pl.ds(768 * p, 768)], w)
        normed = normed2[rows, :].astype(F32)
        column_sum(1, grad * normed)
        column_sum(2, grad)
        start = total[rows, :] + norm_step(grad, normed, rstd2[rows, 0:1], vec[1:2, :])
        m = mask[rows, 0:1]
        column_sum(0, start * m)
        mixed[rows, :] = (start * (1.0 - m)).astype(BF)
        return carry

    lax.fori_loop(0, 2, norm1, 0)
    svc.call()
    lax.fori_loop(2, 4, norm1, 0)
    svc.call()
    load("patch", mixed, patch_out)
    small_stage = 0
    while svc.busy() or small_stage < 5:
        if small_stage == 0:
            r.small_stage(0, sums[...])
        elif small_stage < 4:
            r.small_stage(small_stage)
        elif small_stage == 4:
            small_out[...] = r.small_stage(4)
        small_stage += 1
        svc.call()
    loaded("patch")
    r.finish()


def backward_call(vec, mask, held, full):
    scratch = [
        pltpu.VMEM((1024, 768), BF),
        pltpu.VMEM((1024, 2304), BF),
        pltpu.VMEM((1024, 3072), BF),
        pltpu.VMEM(FULL["fc2"], BF),
        pltpu.VMEM(FULL["fc1"], BF),
        pltpu.VMEM((1024, 768), BF),
        pltpu.VMEM((1024, 768), BF),
        pltpu.VMEM((1024, 128), F32),
        pltpu.VMEM((1024, 768), BF),
        pltpu.VMEM((1024, 768), F32),
        pltpu.VMEM((16, 768), F32),
        pltpu.VMEM((3, 512, 128), F32),
        pltpu.VMEM(FULL["fc2"], BF),
        pltpu.VMEM(FULL["fc1"], BF),
        pltpu.VMEM(FULL["out"], BF),
        pltpu.VMEM((3, 96, 768), BF),
        pltpu.SemaphoreType.DMA((26,)),
        pltpu.SemaphoreType.DMA((NU, 3)),
    ]
    shapes = [jax.ShapeDtypeStruct(SHARD[k], BF) for k in NAMES]
    shapes += [jax.ShapeDtypeStruct((16, 768), F32), jax.ShapeDtypeStruct((1024, 768), BF)]
    return pl.pallas_call(
        backward_kernel,
        out_shape=shapes,
        in_specs=[VM] * 2 + [ANY] * 15,
        out_specs=[ANY] * 4 + [VM, ANY],
        scratch_shapes=scratch + Reduce.SCRATCH,
        compiler_params=kernel_params(1),
        name="backward",
    )(vec, mask, *held, *full)


SHARD = {"qkv": (96, 2304), "out": (96, 768), "fc1": (96, 3072), "fc2": (384, 768)}


def finish_kernel(*refs):
    for source, target in zip(refs[:6], refs[6:]):
        target[...] = source[...].astype(target.dtype)


def finish_call(*arrays):
    kinds = [BF, BF, F32, F32, F32, F32]
    specs = [pl.BlockSpec((a.shape[0] // 2, a.shape[1]), lambda i: (i, 0)) for a in arrays]
    return pl.pallas_call(
        finish_kernel,
        out_shape=[jax.ShapeDtypeStruct(a.shape, k) for a, k in zip(arrays, kinds)],
        grid=(2,),
        in_specs=specs,
        out_specs=specs,
        name="finish",
    )(*arrays)


def compute(patches, cotangent, mask_index, mask_count, gathered):
    (
        embed_full,
        gain_attn,
        shift_attn,
        weight_qkv,
        query_bias,
        value_bias,
        weight_out,
        out_bias,
        gain_mlp,
        shift_mlp,
        weight_fc1,
        fc1_bias,
        weight_fc2,
        fc2_bias,
    ) = gathered
    clip_count, seq_len, feature_count = patches.shape
    row_count = clip_count * seq_len
    slot_ids = lax.broadcasted_iota(jnp.int32, (1, mask_index.shape[1]), 1)
    valid_slots = (slot_ids < mask_count[:, None]).astype(jnp.float32)
    patch_ids = lax.broadcasted_iota(jnp.int32, (1, 1, seq_len), 2)
    onehot = (mask_index[:, :, None] == patch_ids).astype(jnp.float32)
    masked = jnp.einsum("cj,cjp->cp", valid_slots, onehot).reshape(row_count, 1)
    kept_rows = 1.0 - masked
    start_rows = (
        patches.reshape(row_count, feature_count).astype(jnp.float32) * kept_rows
        + masked * embed_full.astype(jnp.float32)[None, :]
    )
    normed_attn, rstd_attn = norm_rows(start_rows)
    attn_in = (
        normed_attn * gain_attn.astype(jnp.float32)[None, :]
        + shift_attn.astype(jnp.float32)[None, :]
    ).astype(jnp.bfloat16)
    qkv_bias = jnp.concatenate([query_bias, jnp.zeros_like(query_bias), value_bias]).astype(
        jnp.float32
    )
    qkv = (
        jnp.dot(attn_in, weight_qkv, preferred_element_type=jnp.float32) + qkv_bias[None, :]
    ).astype(jnp.bfloat16)
    qkv_clips = qkv.reshape(clip_count, seq_len, 3 * feature_count)
    attn_mixed, log_total = lax.map(attend, qkv_clips)
    attn_mixed = attn_mixed.reshape(row_count, feature_count)
    middle = start_rows + (
        jnp.dot(attn_mixed, weight_out, preferred_element_type=jnp.float32)
        + out_bias.astype(jnp.float32)[None, :]
    )
    normed_mlp, rstd_mlp = norm_rows(middle)
    mlp_in = (
        normed_mlp * gain_mlp.astype(jnp.float32)[None, :] + shift_mlp.astype(jnp.float32)[None, :]
    ).astype(jnp.bfloat16)
    hidden = (
        jnp.dot(mlp_in, weight_fc1, preferred_element_type=jnp.float32)
        + fc1_bias.astype(jnp.float32)[None, :]
    )
    activated = jax.nn.gelu(hidden, approximate=False).astype(jnp.bfloat16)
    result = middle + (
        jnp.dot(activated, weight_fc2, preferred_element_type=jnp.float32)
        + fc2_bias.astype(jnp.float32)[None, :]
    )
    output = result.astype(jnp.bfloat16).reshape(clip_count, seq_len, feature_count)
    grad_result = cotangent.reshape(row_count, feature_count)
    grad_w_fc2 = dot_rows(activated, grad_result)
    grad_bias_fc2 = jnp.sum(grad_result.astype(jnp.float32), axis=0)
    grad_act = dot_back(grad_result, weight_fc2)
    gelu_slope = (
        0.5 * (1.0 + lax.erf(hidden * inv_root_two))
        + hidden * jnp.exp(-0.5 * hidden * hidden) * inv_root_tau
    )
    grad_hidden = (grad_act * gelu_slope).astype(jnp.bfloat16)
    grad_w_fc1 = dot_rows(mlp_in, grad_hidden)
    grad_bias_fc1 = jnp.sum(grad_hidden.astype(jnp.float32), axis=0)
    grad_mlp_in = dot_back(grad_hidden, weight_fc1)
    grad_ln2_gain = jnp.sum(grad_mlp_in * normed_mlp, axis=0)
    grad_ln2_bias = jnp.sum(grad_mlp_in, axis=0)
    grad_middle = grad_result.astype(jnp.float32) + norm_back(
        grad_mlp_in, normed_mlp, rstd_mlp, gain_mlp.astype(jnp.float32)
    )
    grad_branch = grad_middle.astype(jnp.bfloat16)
    grad_w_out = dot_rows(attn_mixed, grad_branch)
    grad_bias_out = jnp.sum(grad_branch.astype(jnp.float32), axis=0)
    grad_mixed = dot_back(grad_branch, weight_out).astype(jnp.bfloat16)
    grad_qkv = lax.map(
        attend_back, (qkv_clips, grad_mixed.reshape(clip_count, seq_len, feature_count), log_total)
    )
    grad_qkv = grad_qkv.reshape(row_count, 3 * feature_count)
    grad_w_qkv = dot_rows(attn_in, grad_qkv)
    qkv_sums = jnp.sum(grad_qkv.astype(jnp.float32), axis=0)
    grad_bias_q = qkv_sums[:feature_count]
    grad_bias_v = qkv_sums[2 * feature_count :]
    grad_attn_in = dot_back(grad_qkv, weight_qkv)
    grad_ln1_gain = jnp.sum(grad_attn_in * normed_attn, axis=0)
    grad_ln1_bias = jnp.sum(grad_attn_in, axis=0)
    grad_start = grad_middle + norm_back(
        grad_attn_in, normed_attn, rstd_attn, gain_attn.astype(jnp.float32)
    )
    grad_mask_embed = jnp.sum(grad_start * masked, axis=0)
    patch_grad = (
        (grad_start * kept_rows).astype(jnp.bfloat16).reshape(clip_count, seq_len, feature_count)
    )
    return output, patch_grad, (
        grad_mask_embed,
        grad_ln1_gain,
        grad_ln1_bias,
        grad_w_qkv,
        grad_bias_q,
        grad_bias_v,
        grad_w_out,
        grad_bias_out,
        grad_ln2_gain,
        grad_ln2_bias,
        grad_w_fc1,
        grad_bias_fc1,
        grad_w_fc2,
        grad_bias_fc2,
    )


def plain_gather(shards):
    return tuple(lax.all_gather(s, "wide", axis=0, tiled=True) for s in shards)


def plain_reduce(grads):
    shards = [lax.psum_scatter(g, "wide", scatter_dimension=0, tiled=True) for g in grads]
    return tuple(lax.psum(s.astype(BF), "narrow").astype(F32) for s in shards)


SMALL = (0, 1, 2, 4, 5, 7, 8, 9, 13)
BIG = (3, 6, 10, 12)


def place_small(total):
    place = lax.axis_index("wide")
    mine = lax.dynamic_slice(total, (0, place * 96), (9, 96))
    return mine, lax.dynamic_slice(total[9:13].reshape(3072), (place * 384,), (384,))


def mask_rows(mask_index, mask_count, seq_len):
    slot_ids = lax.broadcasted_iota(jnp.int32, (1, mask_index.shape[1]), 1)
    valid_slots = (slot_ids < mask_count[:, None]).astype(F32)
    patch_ids = lax.broadcasted_iota(jnp.int32, (1, 1, seq_len), 2)
    onehot = (mask_index[:, :, None] == patch_ids).astype(F32)
    return jnp.einsum("cj,cjp->cp", valid_slots, onehot).reshape(-1, 1)


def kernel_layer(patches, cotangent, mask_index, mask_count, *shards):
    masked = mask_rows(mask_index, mask_count, 512)
    rows = jnp.pad(jnp.stack([shards[i] for i in SMALL]), ((0, 0), (0, 32)))
    small = jnp.pad(jnp.concatenate([rows, shards[11].reshape(3, 128)]), ((0, 4), (0, 0)))
    cot = cotangent.reshape(1024, 768)
    results = forward_call(patches.reshape(1024, 768), masked, cot, *[shards[i] for i in BIG], small)
    full, kept = results[:4], results[4:]
    *blocks, total, patch_grad = backward_call(kept[11], masked, (cot,) + tuple(kept[:10]), full)
    output, patch_grad, *blocks = finish_call(kept[10], patch_grad, *blocks)
    mine, bias_fc1 = place_small(total)
    grads = [None] * 14
    for row, i in enumerate(SMALL):
        grads[i] = mine[row]
    for i, block in zip(BIG, blocks):
        grads[i] = block
    grads[11] = bias_fc1
    return (output.reshape(patches.shape), patch_grad.reshape(patches.shape)) + tuple(grads)


def plain_layer(patches, cotangent, mask_index, mask_count, *shards):
    output, patch_grad, grads = compute(patches, cotangent, mask_index, mask_count, plain_gather(shards))
    return (output, patch_grad) + plain_reduce(grads)


def solution(mesh):
    in_specs = (
        P(("narrow", "wide"), None, None),
        P(("narrow", "wide"), None, None),
        P(("narrow", "wide"), None),
        P(("narrow", "wide")),
        P("wide"),
        P("wide"),
        P("wide"),
        P("wide", None),
        P("wide"),
        P("wide"),
        P("wide", None),
        P("wide"),
        P("wide"),
        P("wide"),
        P("wide", None),
        P("wide"),
        P("wide", None),
        P("wide"),
    )
    out_specs = (
        P(("narrow", "wide"), None, None),
        P(("narrow", "wide"), None, None),
        P("wide"),
        P("wide"),
        P("wide"),
        P("wide", None),
        P("wide"),
        P("wide"),
        P("wide", None),
        P("wide"),
        P("wide"),
        P("wide"),
        P("wide", None),
        P("wide"),
        P("wide", None),
        P("wide"),
    )
    kernels = mesh.shape["narrow"] == 4 and mesh.shape["wide"] == 8
    return jax.shard_map(
        kernel_layer if kernels else plain_layer, mesh=mesh, in_specs=in_specs, out_specs=out_specs, check_vma=False
    )
```
